256 devices in a mesh: exp: 32 (over x, z), dat: 8 (over y, core).
Axes of the slice: x: 4, y: 4, z: 8, core: 2. Of those that a mesh axis runs over, the one named last changes fastest.
Arguments:
- tokens: bfloat16 [32768, 1024], P(('exp', 'dat')), may hold values from -6 to 6
- norm_gain: float32 [1024], replicated, may hold values from 0.25 to 1.75
- router_weight: bfloat16 [1024, 128], P(None, 'exp'), may hold values from -0.1875 to 0.1875
- inner_weight: bfloat16 [128, 1024, 4096], P('exp', None, 'dat'), may hold values from -0.1875 to 0.1875
- outer_weight: bfloat16 [128, 4096, 1024], P('exp', 'dat'), may hold values from -0.09375 to 0.09375
- slot_tokens: int32 [128, 512], P('exp', 'dat'), may hold values from 0 to 32767, as said below
- slot_ids: int32 [32768, 2], P(('exp', 'dat')), may hold values from 0 to 65535, as said below
Outputs:
- mixed: bfloat16 [32768, 1024], P(('exp', 'dat'))
The draws below stay inside these ranges and needn't reach their ends.
Inputs may be any that keep to these rules, and one draw needn't show every extreme that they name: `slot_tokens`: column c of an expert names only tokens of the devices whose dat index is c // 64; one expert names no token twice. The 256 slots of the experts of one exp index in one dat group name tokens of any one device at most 24 times, exactly 24 times for some devices, and no times for some. Every token is named by exactly 2 slots. slot_ids[t] holds the two slots e * 512 + c with slot_tokens[e, c] = t, the smaller first.
All inputs are finite; a program needn't handle non-finite values.
Results may differ from the reference program's by a relative error of at most 0.0085.
Values may be sent and summed in bfloat16 or wider, within the bound.
A program may use at most 64 MiB of HBM per device.

```python
import jax
import jax.numpy as jnp
from jax import lax

D = 1024
FF = 4096
E_DEV = 4
TOK_DEV = 128
E = 128
C_DAT = 64
CAP = 512
TOKENS = 32768
N_EXP = 32
N_DAT = 8


def build_routes(key):
    base = jax.random.fold_in(key, 7)
    groups = N_DAT
    owners = N_EXP
    tok_rows = TOK_DEV
    spread = E_DEV * C_DAT
    average = 2 * TOK_DEV // N_EXP
    ranking = jnp.arange(owners, dtype=jnp.int32)
    profile = jnp.where(ranking < owners // 8, 3 * average, jnp.where(ranking < 3 * owners // 4, average, 0)).astype(jnp.int32)
    key_shift, key_slot, key_token = jax.random.split(base, 3)
    shifts = jax.vmap(lambda subkey: jax.random.permutation(subkey, owners))(jax.random.split(key_shift, groups)).astype(jnp.int32)
    counts = profile[(ranking[None, None, :] + shifts[:, :, None]) % owners]
    after_dev = jnp.cumsum(counts, axis=1)
    start_dev = after_dev - counts
    after_own = jnp.cumsum(counts, axis=2)
    start_own = after_own - counts
    orders = jax.vmap(lambda subkey: jax.random.permutation(subkey, spread))(jax.random.split(key_slot, groups * owners)).reshape(groups, owners, spread).astype(jnp.int32)
    circuits = jax.vmap(lambda subkey: jax.random.permutation(subkey, tok_rows))(jax.random.split(key_token, groups * owners)).reshape(groups, owners, tok_rows).astype(jnp.int32)
    owner_of = jnp.sum((after_own[:, :, None, :] <= orders[:, :, :, None]).astype(jnp.int32), axis=-1)
    within = orders - jnp.take_along_axis(start_own, owner_of, axis=2)
    position = jnp.take_along_axis(start_dev, owner_of, axis=2) + within
    flat_index = (owner_of * tok_rows + position % tok_rows).reshape(groups, owners * spread)
    local_token = jnp.take_along_axis(circuits.reshape(groups, owners * tok_rows), flat_index, axis=1).reshape(groups, owners, spread)
    group_index = jnp.arange(groups, dtype=jnp.int32)[:, None, None]
    token_id = (owner_of * groups + group_index) * tok_rows + local_token
    slot_tokens = token_id.reshape(groups, owners, E_DEV, C_DAT).transpose(1, 2, 0, 3).reshape(owners * E_DEV, groups * C_DAT)
    steps_seq = jnp.arange(2 * tok_rows, dtype=jnp.int32)
    after_by_owner = after_dev.transpose(0, 2, 1)
    device_of = jnp.sum((after_by_owner[:, :, None, :] <= steps_seq[None, None, :, None]).astype(jnp.int32), axis=-1)
    within_dev = steps_seq[None, None, :] - jnp.take_along_axis(start_dev.transpose(0, 2, 1), device_of, axis=2)
    sorted_pos = jnp.take_along_axis(start_own.transpose(0, 2, 1), device_of, axis=2) + within_dev
    inverse = jnp.argsort(orders, axis=-1).astype(jnp.int32)
    flat_slot = (device_of * spread + sorted_pos).reshape(groups, owners * 2 * tok_rows)
    slot_pos = jnp.take_along_axis(inverse.reshape(groups, owners * spread), flat_slot, axis=1).reshape(groups, owners, 2 * tok_rows)
    slot_global = (device_of * E_DEV + slot_pos // C_DAT) * CAP + group_index * C_DAT + slot_pos % C_DAT
    token_place = jnp.argsort(circuits, axis=-1).astype(jnp.int32)
    earlier_id = jnp.take_along_axis(slot_global, token_place, axis=2)
    later_id = jnp.take_along_axis(slot_global, token_place + tok_rows, axis=2)
    paired = jnp.stack([jnp.minimum(earlier_id, later_id), jnp.maximum(earlier_id, later_id)], axis=-1)
    slot_ids = paired.transpose(1, 0, 2, 3).reshape(owners * groups * tok_rows, 2)
    return (slot_tokens.astype(jnp.int32), slot_ids.astype(jnp.int32))


def draw_slot_tokens(key, part):
    return build_routes(key)[0]


def draw_slot_ids(key, part):
    return build_routes(key)[1]


def shard_levels(rng, extent, cuts, smallest, high):
    factor_of, own = 1.0, jax.random.fold_in(rng, 6)
    for dim, blocks in cuts:
        draws = jnp.exp(jax.random.uniform(jax.random.fold_in(own, dim), (blocks,), jnp.float32, smallest / len(cuts), high / len(cuts)))
        factor_of = factor_of * jnp.repeat(draws, extent[dim] // blocks).reshape([-1 if axis == dim else 1 for axis in range(len(extent))])
    return factor_of


def normal_values(own_key, extent, width, bound, cuts=(), kind=jnp.bfloat16):
    values = width * jax.random.normal(own_key, extent, jnp.float32)
    if cuts:
        values = values * shard_levels(own_key, extent, cuts, -0.22, 0.18)
    return jnp.clip(values, -bound, bound).astype(kind)


def setup_inputs(seed: int = 0) -> dict:
    keys = jax.random.split(jax.random.key(seed), 8)
    tokens = normal_values(keys[0], (TOKENS, D), 1.0, 6.0, ((0, 256),))
    norm_gain = jnp.clip(1.0 + 0.15 * jax.random.normal(keys[1], (D,), jnp.float32), 0.25, 1.75)
    router_weight = normal_values(keys[2], (D, E), D ** -0.5, 0.1875, ((1, 32),))
    inner_weight = normal_values(keys[3], (E, D, FF), D ** -0.5, 0.1875, ((0, 32), (2, 8)))
    outer_weight = normal_values(keys[4], (E, FF, D), FF ** -0.5, 0.09375, ((0, 32), (1, 8)))
    slot_tokens = draw_slot_tokens(jax.random.fold_in(keys[7], 71), 0)
    slot_ids = draw_slot_ids(jax.random.fold_in(keys[7], 71), 0)
    return dict(tokens=tokens, norm_gain=norm_gain, router_weight=router_weight, inner_weight=inner_weight, outer_weight=outer_weight, slot_tokens=slot_tokens, slot_ids=slot_ids)


EPSILON = 1e-06

def reference(tokens, norm_gain, router_weight, inner_weight, outer_weight, slot_tokens, slot_ids):
    values = tokens.astype(jnp.float32)
    scale = lax.rsqrt(lax.optimization_barrier(jnp.mean(values * values, axis=-1, keepdims=True)) + EPSILON)
    normed = (values * scale * norm_gain.astype(jnp.float32)).astype(jnp.bfloat16)
    slot_rows = jnp.take(normed, slot_tokens, axis=0)
    gate_score = jax.nn.sigmoid(jnp.einsum('ecd,de->ec', slot_rows.astype(jnp.float32), router_weight.astype(jnp.float32)))
    capacity = slot_tokens.shape[1]
    ff_block = FF // N_DAT

    def expert(inputs):
        block, first_weight, second_weight = inputs
        hidden = jax.nn.relu(jnp.dot(block, first_weight, preferred_element_type=jnp.float32)).astype(jnp.bfloat16)
        pieces = hidden.reshape(capacity, N_DAT, ff_block).astype(jnp.float32)
        seconds = second_weight.reshape(N_DAT, ff_block, D).astype(jnp.float32)
        partial_sums = jnp.einsum('ckf,kfd->kcd', pieces, seconds).astype(jnp.bfloat16)
        partial_sums = lax.optimization_barrier(partial_sums)
        return lax.optimization_barrier(jnp.sum(partial_sums.astype(jnp.float32), axis=0))
    expert_out = lax.map(expert, (slot_rows, inner_weight, outer_weight))
    weighted = (gate_score[:, :, None] * expert_out).astype(jnp.bfloat16).reshape(-1, D)
    chosen = jnp.take(weighted, slot_ids.reshape(-1), axis=0).reshape(slot_ids.shape[0], 2, D).astype(jnp.float32)
    combined = chosen[:, 0] + chosen[:, 1]
    return (values + combined).astype(jnp.bfloat16)
```

```python
import functools

import jax
import jax.numpy as jnp
from jax import lax
from jax.experimental import pallas as pl
from jax.experimental.pallas import tpu as pltpu
from jax.sharding import PartitionSpec as P

EPSILON = 1e-06
MESH = pl.DeviceIdType.MESH
BF16 = jnp.bfloat16
F32 = jnp.float32


def normalize(tokens, norm_gain):
    values = tokens.astype(jnp.float32)
    scale = lax.rsqrt(jnp.mean(values * values, axis=-1, keepdims=True) + EPSILON)
    return (values * scale * norm_gain).astype(jnp.bfloat16)


def owner_places(slot_ids, experts_dev, capacity, bucket):
    flat_ids = slot_ids.reshape(-1)
    source = flat_ids // capacity // experts_dev
    before = (source[:, None] == source[None, :]) & (flat_ids[None, :] < flat_ids[:, None])
    ranks_in = jnp.sum(before.astype(jnp.int32), axis=1)
    return (source * bucket + ranks_in).reshape(slot_ids.shape)


def expert_places(token_ids, slot_keys, tok_rows, dat_count, bucket):
    owner_of = token_ids // (tok_rows * dat_count)
    before = (owner_of[:, None] == owner_of[None, :]) & (slot_keys[None, :] < slot_keys[:, None])
    ranks_in = jnp.sum(before.astype(jnp.int32), axis=1)
    return owner_of * bucket + ranks_in


def ffn_kernel(
    rows, router, w1_hbm, w2_hbm, out,
    X, W1, W2, PS, R, S, T, F,
    w_sem, sendP, recvP, sendI, recvI, rsend, rrecv, fsend, frecv, tsend, trecv,
):
    experts, C, width = rows.shape
    dat = lax.axis_index("dat")
    c, y = dat % 2, dat // 2
    partner = y * 2 + (1 - c)
    plus = ((y + 1) % 4) * 2 + c
    minus = ((y + 3) % 4) * 2 + c
    half = experts // 2

    weights = []
    for e in range(experts):
        weights.append(pltpu.make_async_copy(w1_hbm.at[e], W1.at[e], w_sem.at[0, e]))
        weights.append(pltpu.make_async_copy(w2_hbm.at[e], W2.at[e], w_sem.at[1, e]))
    for copy in weights:
        copy.start()

    barrier = pltpu.get_barrier_semaphore()
    for other in (partner, plus, minus):
        pl.semaphore_signal(barrier, inc=1, device_id={"dat": other}, device_id_type=MESH)
    pl.semaphore_wait(barrier, 3)

    def remote(src, dst, send, recv, where):
        return pltpu.make_async_remote_copy(
            src_ref=src, dst_ref=dst, send_sem=send, recv_sem=recv, device_id={"dat": where}, device_id_type=MESH
        )

    own = pl.ds(0, C)
    other_rows = pl.ds(C, C)

    def to_plus(e):
        return remote(rows.at[e], X.at[1, e, own], sendI.at[1, e], recvI.at[1, e], plus)

    def to_minus(e):
        return remote(rows.at[e], X.at[2, e, own], sendI.at[2, e], recvI.at[2, e], minus)

    def to_partner(s, e):
        src = rows.at[e] if s == 0 else X.at[s, e, own]
        return remote(src, X.at[s, e, other_rows], sendP.at[s, e], recvP.at[s, e], partner)

    def onward(e):
        if e < half:
            return remote(X.at[1, e, own], X.at[3, e, own], sendI.at[3, e], recvI.at[3, e], plus)
        return remote(X.at[2, e, own], X.at[3, e, own], sendI.at[3, e], recvI.at[3, e], minus)

    def part_to_partner(s, e):
        return remote(PS.at[s, e, other_rows], R.at[s, e], rsend.at[s, e], rrecv.at[s, e], partner)

    def final_plus(e):
        return remote(S.at[2, e], F.at[0, e], fsend.at[0, e], frecv.at[0, e], plus)

    def final_minus(e):
        return remote(S.at[1, e], F.at[1, e], fsend.at[1, e], frecv.at[1, e], minus)

    def transit(e):
        where = plus if e < half else minus
        return remote(S.at[3, e], T.at[e], tsend.at[e], trecv.at[e], where)

    def ffn(s, e):
        inner = jnp.dot(X[s, e], W1[e], preferred_element_type=F32)
        hidden = jnp.maximum(inner, 0.0).astype(BF16)
        PS[s, e] = jnp.dot(hidden, W2[e], preferred_element_type=F32).astype(BF16)

    def chip_sum(s, e):
        part_to_partner(s, e).wait_recv()
        return PS[s, e, :C].astype(F32) + R[s, e].astype(F32)

    for k in range(experts):
        to_plus(k).start()
        to_minus((k + half) % experts).start()
    for k in range(experts):
        to_partner(0, k).start()
    for e in range(experts):
        X[0, e, :C] = rows[e]

    def first(e, carry):
        remote(rows.at[e], X.at[0, e, other_rows], sendP.at[0, e], recvP.at[0, e], partner).wait_recv()
        pltpu.make_async_copy(w1_hbm.at[e], W1.at[e], w_sem.at[0, e]).wait()
        pltpu.make_async_copy(w2_hbm.at[e], W2.at[e], w_sem.at[1, e]).wait()
        ffn(0, e)
        part_to_partner(0, e).start()
        return carry

    lax.fori_loop(0, experts, first, 0)

    def arrivals(k):
        if k < experts:
            return [(1, k), (2, (k + half) % experts)]
        if k < experts + half:
            return [(3, k - experts), (3, k - experts + half)]
        return []

    def receive(s, e):
        src = rows.at[e] if s < 3 else X.at[1, e, own]
        remote(src, X.at[s, e, own], sendI.at[s, e], recvI.at[s, e], partner).wait_recv()
        to_partner(s, e).start()
        if (s == 1 and e < half) or (s == 2 and e >= half):
            onward(e).start()

    def compute(pairs):
        for s, e in pairs:
            to_partner(s, e).wait_recv()
        (s0, e0), (s1, e1) = pairs

        def one(i, carry):
            ffn(s0 + (s1 - s0) * i, e0 + (e1 - e0) * i)
            return carry

        lax.fori_loop(0, 2, one, 0)
        for s, e in pairs:
            part_to_partner(s, e).start()

    def settle(pairs):
        for s, e in pairs:
            S[s, e] = chip_sum(s, e).astype(BF16)
            if s == 3:
                transit(e).start()
            elif s == 1 and e < half:
                final_minus(e).start()
            elif s == 2 and e >= half:
                final_plus(e).start()

    for k in range(experts + half + 2):
        for s, e in arrivals(k):
            receive(s, e)
        if k >= 1 and arrivals(k - 1):
            compute(arrivals(k - 1))
        if k >= 2 and arrivals(k - 2):
            settle(arrivals(k - 2))

    for k in range(half):
        a, b = k, k + half
        transit(a).wait_recv()
        S[2, a] = (S[2, a].astype(F32) + T[a].astype(F32)).astype(BF16)
        final_plus(a).start()
        transit(b).wait_recv()
        S[1, b] = (S[1, b].astype(F32) + T[b].astype(F32)).astype(BF16)
        final_minus(b).start()

    for e in list(range(half, experts)) + list(range(half)):
        logits = jnp.sum(rows[e].astype(F32) * router[e : e + 1].astype(F32), axis=1, keepdims=True)
        gate = jax.nn.sigmoid(logits)
        total = chip_sum(0, e)
        final_plus(e).wait_recv()
        final_minus(e).wait_recv()
        total = total + F[0, e].astype(F32) + F[1, e].astype(F32)
        out[e] = (gate * total).astype(BF16)

    for e in range(experts):
        to_plus(e).wait_send()
        to_minus(e).wait_send()
        onward(e).wait_send()
        final_plus(e).wait_send()
        final_minus(e).wait_send()
        transit(e).wait_send()
        for s in range(4):
            to_partner(s, e).wait_send()
            part_to_partner(s, e).wait_send()


def expert_layer(rows, router, inner_weight, outer_weight):
    experts, C, width = rows.shape
    hidden = inner_weight.shape[2]
    dma = pltpu.SemaphoreType.DMA
    vmem = pl.BlockSpec(memory_space=pltpu.VMEM)
    hbm = pl.BlockSpec(memory_space=pl.ANY)
    return pl.pallas_call(
        ffn_kernel,
        name="expert_layer",
        out_shape=jax.ShapeDtypeStruct((experts, C, width), BF16),
        in_specs=[vmem, vmem, hbm, hbm],
        out_specs=vmem,
        scratch_shapes=[
            pltpu.VMEM((4, experts, 2 * C, width), BF16),
            pltpu.VMEM((experts, width, hidden), BF16),
            pltpu.VMEM((experts, hidden, width), BF16),
            pltpu.VMEM((4, experts, 2 * C, width), BF16),
            pltpu.VMEM((4, experts, C, width), BF16),
            pltpu.VMEM((4, experts, C, width), BF16),
            pltpu.VMEM((experts, C, width), BF16),
            pltpu.VMEM((2, experts, C, width), BF16),
            dma((2, experts)),
            dma((4, experts)),
            dma((4, experts)),
            dma((4, experts)),
            dma((4, experts)),
            dma((4, experts)),
            dma((4, experts)),
            dma((2, experts)),
            dma((2, experts)),
            dma((experts,)),
            dma((experts,)),
        ],
        compiler_params=pltpu.CompilerParams(
            collective_id=0, has_side_effects=True, vmem_limit_bytes=60 * 1024 * 1024
        ),
    )(rows, router, inner_weight, outer_weight)


def body(tokens, norm_gain, router_weight, inner_weight, outer_weight, slot_tokens, slot_ids):
    exp_count = lax.axis_size("exp")
    dat_count = lax.axis_size("dat")
    tok_rows, width = tokens.shape
    experts_dev, cap_dev = slot_tokens.shape
    bucket = 6 * tok_rows // exp_count
    normed = normalize(tokens, norm_gain)
    picked = slot_tokens.reshape(-1)
    slot_keys = lax.iota(jnp.int32, experts_dev * cap_dev)
    senders = expert_places(picked, slot_keys, tok_rows, dat_count, bucket)
    receivers = owner_places(slot_ids, experts_dev, cap_dev * dat_count, bucket)
    lookup = jnp.any(
        lax.broadcasted_iota(jnp.int32, (exp_count * bucket, 1, 1), 0) == receivers[None], axis=2
    )
    outgoing = jnp.dot(lookup.astype(BF16), normed, preferred_element_type=F32)
    outgoing = outgoing.astype(BF16).reshape(exp_count, bucket, width)
    arrived = lax.all_to_all(outgoing, "exp", split_axis=0, concat_axis=0, tiled=True).reshape(
        exp_count * bucket, width
    )
    placing = lax.broadcasted_iota(jnp.int32, (exp_count * bucket, 1), 0) == senders[None, :]
    placing = placing.astype(BF16)
    gathered_rows = lax.dot_general(
        placing, arrived, (((0,), (0,)), ((), ())), preferred_element_type=F32
    ).astype(BF16)
    gathered_rows = gathered_rows.reshape(experts_dev, cap_dev, width)
    weighted = expert_layer(gathered_rows, router_weight.T, inner_weight, outer_weight)
    weighted = weighted.reshape(-1, width)
    returning = jnp.dot(placing, weighted, preferred_element_type=F32)
    returning = returning.astype(BF16).reshape(exp_count, bucket, width)
    came_back = lax.all_to_all(returning, "exp", split_axis=0, concat_axis=0, tiled=True).reshape(
        exp_count * bucket, width
    )
    combine_table = jnp.sum(
        (lax.broadcasted_iota(jnp.int32, (1, 1, exp_count * bucket), 2) == receivers[:, :, None]).astype(F32),
        axis=1,
    )
    combined = jnp.dot(combine_table.astype(BF16), came_back, preferred_element_type=F32)
    return (tokens.astype(F32) + combined).astype(BF16)


def solution(mesh):
    in_specs = (
        P(("exp", "dat"), None),
        P(),
        P(None, "exp"),
        P("exp", None, "dat"),
        P("exp", "dat", None),
        P("exp", "dat"),
        P(("exp", "dat"), None),
    )
    out_specs = P(("exp", "dat"), None)
    return jax.shard_map(body, mesh=mesh, in_specs=in_specs, out_specs=out_specs, check_vma=False)
```

```python
import functools

import jax
import jax.numpy as jnp
from jax import lax
from jax.experimental import pallas as pl
from jax.experimental.pallas import tpu as pltpu
from jax.sharding import PartitionSpec as P

EPSILON = 1e-06
MESH = pl.DeviceIdType.MESH
BF16 = jnp.bfloat16
F32 = jnp.float32


NX, NZ = 4, 8
BUCKET = 24


def dot(a, b):
    return jnp.dot(a, b, preferred_element_type=F32)


def lane_rows(column_code, width):
    return jnp.transpose(jnp.broadcast_to(column_code, (width, width)))


class Exchange:
    def __init__(self, refs, width):
        self.__dict__.update(refs)
        exp = lax.axis_index("exp")
        self.x, self.z = exp // NZ, exp % NZ
        self.half = width // 2

    def at(self, dx, dz):
        return ((self.x + dx) % NX) * NZ + (self.z + dz) % NZ

    def peers(self):
        return [self.at(0, dz) for dz in range(1, NZ)] + [self.at(1, 0), self.at(NX - 1, 0)]

    def remote(self, src, dst, send, recv, where):
        return pltpu.make_async_remote_copy(
            src_ref=src, dst_ref=dst, send_sem=send, recv_sem=recv, device_id={"exp": where}, device_id_type=MESH
        )

    def cols(self, h):
        return pl.ds(h * self.half, self.half)

    def spread(self, j, h, up):
        src = self.G.at[(j - 1) if up else (j + 1) % NZ, h]
        where = self.at(0, 1) if up else self.at(0, NZ - 1)
        return self.remote(src, self.G.at[j, h], self.gsend.at[j, h], self.grecv.at[j, h], where)

    def code(self, j):
        return self.remote(self.C.at[0], self.C.at[j], self.csend.at[j], self.crecv.at[j], self.at(0, j))

    def bucket(self, ph, j, kind):
        into, through = (self.A, self.TA) if ph == 0 else (self.B, self.TB)

        def lead(i):
            return into.at[i, j] if ph == 0 else into.at[j, i]

        send, recv = self.xsend.at[ph, j, kind], self.xrecv.at[ph, j, kind]
        up, down = self.at(1, 0), self.at(NX - 1, 0)
        if kind == 0:
            return self.remote(self.Q.at[ph, j, 0], lead(3), send, recv, up)
        if kind == 1:
            return self.remote(self.Q.at[ph, j, 1], lead(1), send, recv, down)
        h = kind % 2
        where = down if h else up
        if kind < 4:
            return self.remote(self.QH.at[ph, j, h], through.at[j, h], send, recv, where)
        dst = lead(2).at[:, self.cols(h)]
        return self.remote(through.at[j, h], dst, send, recv, where)

    def send_buckets(self, ph, j, rows):
        n = BUCKET
        for h in range(2):
            self.QH[ph, j, h] = rows[2 * n : 3 * n, h * self.half : (h + 1) * self.half]
            self.bucket(ph, j, 2 + h).start()
        self.Q[ph, j, 0] = rows[n : 2 * n]
        self.bucket(ph, j, 0).start()
        self.Q[ph, j, 1] = rows[3 * n :]
        self.bucket(ph, j, 1).start()
        if ph == 0:
            self.A[0, j] = rows[:n]
        else:
            self.B[j, 0] = rows[:n]

    def relay(self, ph, j):
        for h in range(2):
            self.bucket(ph, j, 2 + h).wait_recv()
            self.bucket(ph, j, 4 + h).start()

    def wait_buckets(self, ph, j):
        for kind in (0, 1, 4, 5):
            self.bucket(ph, j, kind).wait_recv()

    def row_codes(self, shape, dim):
        line = lax.broadcasted_iota(jnp.int32, shape, dim)
        dx = sum((line >= BUCKET * k).astype(jnp.int32) for k in (1, 2, 3))
        rank = line - BUCKET * dx
        owner = ((self.x + dx) % NX) * NZ + self.z
        return jnp.where(line < BUCKET * NX, owner * BUCKET + rank, -7)

    def select(self, j):
        rows = self.row_codes((NX * BUCKET, self.C.shape[2]), 0)
        hit = (rows == self.C[j, 0:1]) | (rows == self.C[j, 1:2])
        hit = hit.astype(F32).astype(BF16)
        left, right = dot(hit, self.G[j, 0]), dot(hit, self.G[j, 1])
        self.send_buckets(0, j, jnp.concatenate([left, right], axis=1).astype(BF16))

    def dispatch(self, tokens, gain, pos, rows):
        values = tokens[...].astype(F32)
        scale = lax.rsqrt(jnp.mean(values * values, axis=-1, keepdims=True) + EPSILON)
        normed = (values * scale * gain[...]).astype(BF16)
        for h in range(2):
            self.G[0, h] = normed[:, h * self.half : (h + 1) * self.half]
            self.spread(1, h, True).start()
            self.spread(NZ - 1, h, False).start()
        for j in range(1, NZ):
            self.code(j).start()
        self.select(0)
        for s in (1, 2, 3):
            for h in range(2):
                self.spread(s, h, True).wait_recv()
                if s < 3 or h == 0:
                    self.spread(s + 1, h, True).start()
                self.spread(NZ - s, h, False).wait_recv()
                if s < 3 or h == 1:
                    self.spread(NZ - s - 1, h, False).start()
            for j in (0,) if s == 1 else (s - 1, NZ - s + 1):
                self.relay(0, j)
            for j in (s, NZ - s):
                self.code(j).wait_recv()
                self.select(j)
        self.code(4).wait_recv()
        self.spread(4, 0, True).wait_recv()
        self.spread(4, 1, False).wait_recv()
        self.select(4)
        for j in (3, 5, 4):
            self.relay(0, j)
        experts, cap, width = rows.shape
        blocks = []
        for b in range(2):
            places = lane_rows(pos[0:1, b * 128 : (b + 1) * 128], 128)[:, :1]
            blocks.append(places)
        for j in range(NZ):
            self.wait_buckets(0, j)
        count = NX * NZ * BUCKET
        arrived = self.A[...].reshape(count, width)
        for b, places in enumerate(blocks):
            hit = (places == lax.broadcasted_iota(jnp.int32, (128, count), 1)).astype(F32).astype(BF16)
            got = dot(hit, arrived).astype(BF16)
            per = 128 // cap
            for i in range(per):
                rows[b * per + i] = got[i * cap : (i + 1) * cap]

    def expanders(self):
        codes = self.row_codes((128, 128), 1)
        for j in range(NZ):
            first, second = lane_rows(self.C[j, 0:1], 128), lane_rows(self.C[j, 1:2], 128)
            self.OT[j] = ((first == codes) | (second == codes)).astype(F32).astype(BF16)

    def give_back(self, tokens, pos, weighted, out):
        experts, cap, width = weighted.shape
        slots = experts * cap
        n = NX * BUCKET
        line = lax.broadcasted_iota(jnp.int32, (n, slots), 0)
        dx = sum((line >= BUCKET * k).astype(jnp.int32) for k in (1, 2, 3))
        base = dx * (NZ * BUCKET) + (line - BUCKET * dx)

        def send(j):
            hit = (base + j * BUCKET == pos[0:1, :]).astype(F32).astype(BF16)
            self.send_buckets(1, j, dot(hit, weighted[...].reshape(slots, width)).astype(BF16))

        def landed(j):
            self.wait_buckets(1, j)

        def part(j, h):
            rows = self.B[j, :, :, h * self.half : (h + 1) * self.half].reshape(n, self.half)
            return dot(self.OT[j][:, :n], rows)

        def fold(j, h, up):
            where, way = (self.at(0, 1), 0) if up else (self.at(0, NZ - 1), 1)
            there = (j + 1) % NZ if up else j - 1
            return self.remote(
                self.V.at[j, h], self.RP.at[way, there, h],
                self.vsend.at[j, h], self.vrecv.at[way, there, h], where,
            )

        def got(j, h, up):
            fold((j - 1) % NZ if up else j + 1, h, up).wait_recv()
            return self.RP[0 if up else 1, j, h].astype(F32)

        def emit(j, h, up, incoming):
            value = part(j, h)
            if incoming:
                value = value + got(j, h, up)
            self.V[j, h] = value.astype(BF16)
            fold(j, h, up).start()

        send(4)
        send(5)
        send(3)
        self.relay(1, 4)
        landed(4)
        emit(4, 0, True, False)
        emit(4, 1, False, False)
        for s, ahead in ((1, (6, 2)), (2, (7, 1)), (3, (0,))):
            for j in ahead:
                send(j)
            up, down = 4 + s, 4 - s
            for j in (up, down):
                self.relay(1, j)
            for j in (up, down):
                landed(j)
            emit(up, 1, True, s > 1)
            emit(down, 0, False, s > 1)
            emit(up, 0, True, True)
            emit(down, 1, False, True)
        self.relay(1, 0)
        landed(0)
        for h in (1, 0):
            cut = slice(h * self.half, (h + 1) * self.half)
            total = tokens[:, cut].astype(F32) + part(0, h)
            total = total + got(0, h, True) + got(0, h, False)
            out[:, cut] = total.astype(BF16)
        for ph in range(2):
            for j in range(NZ):
                for kind in range(6):
                    self.bucket(ph, j, kind).wait_send()
        for j in range(1, NZ):
            self.code(j).wait_send()
            for h in range(2):
                up = j < 4 or (j == 4 and h == 0)
                self.spread(j, h, up).wait_send()
                fold(j, h, j > 4 or (j == 4 and h == 0)).wait_send()


def exchange_scratch(tok_rows, width):
    dma = pltpu.SemaphoreType.DMA
    half = width // 2
    return dict(
        G=pltpu.VMEM((NZ, 2, tok_rows, half), BF16),
        C=pltpu.VMEM((NZ, 8, tok_rows), jnp.int32),
        Q=pltpu.VMEM((2, NZ, 2, BUCKET, width), BF16),
        QH=pltpu.VMEM((2, NZ, 2, BUCKET, half), BF16),
        A=pltpu.VMEM((NX, NZ, BUCKET, width), BF16),
        B=pltpu.VMEM((NZ, NX, BUCKET, width), BF16),
        TA=pltpu.VMEM((NZ, 2, BUCKET, half), BF16),
        TB=pltpu.VMEM((NZ, 2, BUCKET, half), BF16),
        OT=pltpu.VMEM((NZ, 128, 128), BF16),
        V=pltpu.VMEM((NZ, 2, tok_rows, half), BF16),
        RP=pltpu.VMEM((2, NZ, 2, tok_rows, half), BF16),
        gsend=dma((NZ, 2)),
        grecv=dma((NZ, 2)),
        csend=dma((NZ,)),
        crecv=dma((NZ,)),
        xsend=dma((2, NZ, 6)),
        xrecv=dma((2, NZ, 6)),
        vsend=dma((NZ, 2)),
        vrecv=dma((2, NZ, 2)),
    )


def expert_layer(
    rows, router, w1_hbm, w2_hbm, out, meanwhile,
    X, W1, W2, PS, R, S, T, F,
    w_sem, sendP, recvP, sendI, recvI, rsend, rrecv, fsend, frecv, tsend, trecv,
):
    experts, C, width = rows.shape
    dat = lax.axis_index("dat")
    c, y = dat % 2, dat // 2
    partner = y * 2 + (1 - c)
    plus = ((y + 1) % 4) * 2 + c
    minus = ((y + 3) % 4) * 2 + c
    half = experts // 2

    def remote(src, dst, send, recv, where):
        return pltpu.make_async_remote_copy(
            src_ref=src, dst_ref=dst, send_sem=send, recv_sem=recv, device_id={"dat": where}, device_id_type=MESH
        )

    own = pl.ds(0, C)
    other_rows = pl.ds(C, C)

    def to_plus(e):
        return remote(rows.at[e], X.at[1, e, own], sendI.at[1, e], recvI.at[1, e], plus)

    def to_minus(e):
        return remote(rows.at[e], X.at[2, e, own], sendI.at[2, e], recvI.at[2, e], minus)

    def to_partner(s, e):
        src = rows.at[e] if s == 0 else X.at[s, e, own]
        return remote(src, X.at[s, e, other_rows], sendP.at[s, e], recvP.at[s, e], partner)

    def onward(e):
        if e < half:
            return remote(X.at[1, e, own], X.at[3, e, own], sendI.at[3, e], recvI.at[3, e], plus)
        return remote(X.at[2, e, own], X.at[3, e, own], sendI.at[3, e], recvI.at[3, e], minus)

    def part_to_partner(s, e):
        return remote(PS.at[s, e, other_rows], R.at[s, e], rsend.at[s, e], rrecv.at[s, e], partner)

    def final_plus(e):
        return remote(S.at[2, e], F.at[0, e], fsend.at[0, e], frecv.at[0, e], plus)

    def final_minus(e):
        return remote(S.at[1, e], F.at[1, e], fsend.at[1, e], frecv.at[1, e], minus)

    def transit(e):
        where = plus if e < half else minus
        return remote(S.at[3, e], T.at[e], tsend.at[e], trecv.at[e], where)

    def ffn(s, e):
        inner = jnp.dot(X[s, e], W1[e], preferred_element_type=F32)
        hidden = jnp.maximum(inner, 0.0).astype(BF16)
        PS[s, e] = jnp.dot(hidden, W2[e], preferred_element_type=F32).astype(BF16)

    def chip_sum(s, e):
        part_to_partner(s, e).wait_recv()
        return PS[s, e, :C].astype(F32) + R[s, e].astype(F32)

    for k in range(experts):
        to_plus(k).start()
        to_minus((k + half) % experts).start()
    for k in range(experts):
        to_partner(0, k).start()
    for e in range(experts):
        X[0, e, :C] = rows[e]
    meanwhile()

    def first(e, carry):
        remote(rows.at[e], X.at[0, e, other_rows], sendP.at[0, e], recvP.at[0, e], partner).wait_recv()
        pltpu.make_async_copy(w1_hbm.at[e], W1.at[e], w_sem.at[0, e]).wait()
        pltpu.make_async_copy(w2_hbm.at[e], W2.at[e], w_sem.at[1, e]).wait()
        ffn(0, e)
        part_to_partner(0, e).start()
        return carry

    lax.fori_loop(0, experts, first, 0)

    def arrivals(k):
        if k < experts:
            return [(1, k), (2, (k + half) % experts)]
        if k < experts + half:
            return [(3, k - experts), (3, k - experts + half)]
        return []

    def receive(s, e):
        src = rows.at[e] if s < 3 else X.at[1, e, own]
        remote(src, X.at[s, e, own], sendI.at[s, e], recvI.at[s, e], partner).wait_recv()
        to_partner(s, e).start()
        if (s == 1 and e < half) or (s == 2 and e >= half):
            onward(e).start()

    def compute(pairs):
        for s, e in pairs:
            to_partner(s, e).wait_recv()
        (s0, e0), (s1, e1) = pairs

        def one(i, carry):
            ffn(s0 + (s1 - s0) * i, e0 + (e1 - e0) * i)
            return carry

        lax.fori_loop(0, 2, one, 0)
        for s, e in pairs:
            part_to_partner(s, e).start()

    def settle(pairs):
        for s, e in pairs:
            S[s, e] = chip_sum(s, e).astype(BF16)
            if s == 3:
                transit(e).start()
            elif s == 1 and e < half:
                final_minus(e).start()
            elif s == 2 and e >= half:
                final_plus(e).start()

    for k in range(experts + half + 2):
        for s, e in arrivals(k):
            receive(s, e)
        if k >= 1 and arrivals(k - 1):
            compute(arrivals(k - 1))
        if k >= 2 and arrivals(k - 2):
            settle(arrivals(k - 2))

    for k in range(half):
        a, b = k, k + half
        transit(a).wait_recv()
        S[2, a] = (S[2, a].astype(F32) + T[a].astype(F32)).astype(BF16)
        final_plus(a).start()
        transit(b).wait_recv()
        S[1, b] = (S[1, b].astype(F32) + T[b].astype(F32)).astype(BF16)
        final_minus(b).start()

    for e in list(range(half, experts)) + list(range(half)):
        logits = jnp.sum(rows[e].astype(F32) * router[e : e + 1].astype(F32), axis=1, keepdims=True)
        gate = jax.nn.sigmoid(logits)
        total = chip_sum(0, e)
        final_plus(e).wait_recv()
        final_minus(e).wait_recv()
        total = total + F[0, e].astype(F32) + F[1, e].astype(F32)
        out[e] = (gate * total).astype(BF16)

    for e in range(experts):
        to_plus(e).wait_send()
        to_minus(e).wait_send()
        onward(e).wait_send()
        final_plus(e).wait_send()
        final_minus(e).wait_send()
        transit(e).wait_send()
        for s in range(4):
            to_partner(s, e).wait_send()
            part_to_partner(s, e).wait_send()


def expert_scratch(experts, C, width, hidden):
    dma = pltpu.SemaphoreType.DMA
    return dict(
        X=pltpu.VMEM((4, experts, 2 * C, width), BF16),
        W1=pltpu.VMEM((experts, width, hidden), BF16),
        W2=pltpu.VMEM((experts, hidden, width), BF16),
        PS=pltpu.VMEM((4, experts, 2 * C, width), BF16),
        R=pltpu.VMEM((4, experts, C, width), BF16),
        S=pltpu.VMEM((4, experts, C, width), BF16),
        T=pltpu.VMEM((experts, C, width), BF16),
        F=pltpu.VMEM((2, experts, C, width), BF16),
        w_sem=dma((2, experts)),
        sendP=dma((4, experts)),
        recvP=dma((4, experts)),
        sendI=dma((4, experts)),
        recvI=dma((4, experts)),
        rsend=dma((4, experts)),
        rrecv=dma((4, experts)),
        fsend=dma((2, experts)),
        frecv=dma((2, experts)),
        tsend=dma((experts,)),
        trecv=dma((experts,)),
    )


def layer_kernel(names, with_experts, tokens, gain, codes, pos, router, w1_hbm, w2_hbm, out, rows, weighted, *refs):
    refs = dict(zip(names, refs))
    width = tokens.shape[1]
    experts = rows.shape[0]
    mine = {k: refs.pop(k) for k in exchange_scratch(8, 8)}
    exchange = Exchange(mine, width)
    if with_experts:
        for e in range(experts):
            pltpu.make_async_copy(w1_hbm.at[e], refs["W1"].at[e], refs["w_sem"].at[0, e]).start()
            pltpu.make_async_copy(w2_hbm.at[e], refs["W2"].at[e], refs["w_sem"].at[1, e]).start()
    dat = lax.axis_index("dat")
    c, y = dat % 2, dat // 2
    barrier = pltpu.get_barrier_semaphore()
    others = [{"exp": where} for where in exchange.peers()]
    if with_experts:
        others += [{"dat": y * 2 + 1 - c}, {"dat": ((y + 1) % 4) * 2 + c}, {"dat": ((y + 3) % 4) * 2 + c}]
    for other in others:
        pl.semaphore_signal(barrier, inc=1, device_id=other, device_id_type=MESH)
    exchange.C[0] = codes[...]
    pl.semaphore_wait(barrier, len(others))
    exchange.dispatch(tokens, gain, pos, rows)
    if with_experts:
        expert_layer(rows, router, w1_hbm, w2_hbm, weighted, exchange.expanders, **refs)
    else:
        exchange.expanders()
        for e in range(experts):
            weighted[e] = rows[e]
    exchange.give_back(tokens, pos, weighted, out)


def whole_layer(tokens, gain, codes, pos, router, inner_weight, outer_weight, with_experts=True):
    tok_rows, width = tokens.shape
    experts, _, hidden = inner_weight.shape
    cap = pos.shape[1] // experts
    vmem = pl.BlockSpec(memory_space=pltpu.VMEM)
    hbm = pl.BlockSpec(memory_space=pl.ANY)
    scratch = exchange_scratch(tok_rows, width)
    if with_experts:
        scratch.update(expert_scratch(experts, cap, width, hidden))
    slots = pltpu.VMEM((experts, cap, width), BF16)
    return pl.pallas_call(
        functools.partial(layer_kernel, tuple(scratch), with_experts),
        name="whole_layer",
        out_shape=jax.ShapeDtypeStruct((tok_rows, width), BF16),
        in_specs=[vmem] * 5 + [hbm] * 2,
        out_specs=vmem,
        scratch_shapes=[slots, slots] + list(scratch.values()),
        compiler_params=pltpu.CompilerParams(
            collective_id=0, has_side_effects=True, vmem_limit_bytes=60 * 1024 * 1024
        ),
    )(tokens, gain, codes, pos, router, inner_weight, outer_weight)


def routes(slot_tokens, slot_ids, tok_rows, dat_count):
    experts_dev, cap_dev = slot_tokens.shape
    x, z = lax.axis_index("exp") // NZ, lax.axis_index("exp") % NZ
    flat_ids = slot_ids.T.reshape(-1)
    owner = flat_ids // (experts_dev * cap_dev * dat_count)
    before = (owner[:, None] == owner[None, :]) & (flat_ids[:, None] < flat_ids[None, :])
    codes = owner * BUCKET + jnp.sum(before.astype(jnp.int32), axis=0)
    codes = jnp.pad(codes.reshape(2, tok_rows), ((0, 6), (0, 0)), constant_values=-1)
    picked = slot_tokens.reshape(-1)
    keys = lax.iota(jnp.int32, experts_dev * cap_dev)
    source = picked // (tok_rows * dat_count)
    before = (source[:, None] == source[None, :]) & (keys[:, None] < keys[None, :])
    rank = jnp.sum(before.astype(jnp.int32), axis=0)
    place = ((source // NZ - x) % NX) * NZ + (z - source % NZ) % NZ
    return codes, (place * BUCKET + rank)[None, :]


def body(tokens, norm_gain, router_weight, inner_weight, outer_weight, slot_tokens, slot_ids):
    codes, pos = routes(slot_tokens, slot_ids, tokens.shape[0], lax.axis_size("dat"))
    return whole_layer(tokens, norm_gain[None, :], codes, pos, router_weight.T, inner_weight, outer_weight)


def solution(mesh):
    in_specs = (
        P(("exp", "dat"), None),
        P(),
        P(None, "exp"),
        P("exp", None, "dat"),
        P("exp", "dat", None),
        P("exp", "dat"),
        P(("exp", "dat"), None),
    )
    out_specs = P(("exp", "dat"), None)
    return jax.shard_map(body, mesh=mesh, in_specs=in_specs, out_specs=out_specs, check_vma=False)
```

```python
import functools

import jax
import jax.numpy as jnp
from jax import lax
from jax.experimental import pallas as pl
from jax.experimental.pallas import tpu as pltpu
from jax.sharding import PartitionSpec as P

EPSILON = 1e-06
MESH = pl.DeviceIdType.MESH
BF16 = jnp.bfloat16
F32 = jnp.float32
I32 = jnp.int32

NX, NZ, NY = 4, 8, 4
BUCKET = 24
FAR = NZ // 2


def dot(a, b):
    return jnp.dot(a, b, preferred_element_type=F32)


def onehot(mask):
    return mask.astype(F32).astype(BF16)


def down_rows(row):
    n = row.shape[1]
    return jnp.transpose(jnp.broadcast_to(row, (n, n)))


def count(mask):
    return jnp.sum(mask.astype(F32), axis=0, keepdims=True).astype(I32)


def remote(src, dst, send, recv, where):
    return pltpu.make_async_remote_copy(
        src_ref=src, dst_ref=dst, send_sem=send, recv_sem=recv, device_id=where, device_id_type=MESH
    )


class Exchange:
    def __init__(self, refs, width):
        self.__dict__.update(refs)
        exp = lax.axis_index("exp")
        self.x, self.z = exp // NZ, exp % NZ
        self.chunk, self.piece = width // 2, width // 4

    def at(self, dx, dz):
        return {"exp": ((self.x + dx) % NX) * NZ + (self.z + dz) % NZ}

    def peers(self):
        return [self.at(0, 1), self.at(0, NZ - 1)] + [self.at(dx, 0) for dx in range(1, NX)]

    def routes(self, slot_ids, slot_tokens, tok_rows, slots, dat_count):
        ids = [slot_ids[k : k + 1] for k in range(2)]
        owners = [row // (slots * dat_count) for row in ids]
        for k in range(2):
            rank = 0
            for m in range(2):
                rank = rank + count((down_rows(owners[m]) == owners[k]) & (down_rows(ids[m]) < ids[k]))
            self.C[0, k : k + 1] = owners[k] * BUCKET + rank
        experts = slot_tokens.shape[0]
        per = experts // 2
        source = [
            jnp.concatenate([slot_tokens[b * per + i : b * per + i + 1] for i in range(per)], axis=1)
            // (tok_rows * dat_count)
            for b in range(2)
        ]
        n = slots // 2
        earlier = lax.broadcasted_iota(I32, (n, n), 0) < lax.broadcasted_iota(I32, (n, n), 1)
        for b in range(2):
            rank = count((down_rows(source[b]) == source[b]) & earlier)
            if b == 1:
                rank = rank + count(down_rows(source[0]) == source[1])
            place = ((source[b] // NZ - self.x + NX) % NX) * NZ + (self.z - source[b] % NZ + NZ) % NZ
            self.PO[b : b + 1] = place * BUCKET + rank

    def spread(self, j, p, up):
        src = self.G.at[(j - 1) if up else (j + 1) % NZ, p]
        where = self.at(0, 1) if up else self.at(0, NZ - 1)
        return remote(src, self.G.at[j, p], self.gsend.at[j, p], self.grecv.at[j, p], where)

    def code(self, j):
        up = j <= FAR
        src = self.C.at[(j - 1) if up else (j + 1) % NZ]
        where = self.at(0, 1) if up else self.at(0, NZ - 1)
        return remote(src, self.C.at[j], self.csend.at[j], self.crecv.at[j], where)

    def open_codes(self):
        self.code(1).start()
        self.code(NZ - 1).start()

    def code_hop(self, s):
        self.code(s).wait_recv()
        if s < FAR:
            self.code(s + 1).start()
            self.code(NZ - s).wait_recv()
            if s < FAR - 1:
                self.code(NZ - s - 1).start()

    def bucket(self, ph, q, j, kind):
        def place(i):
            return self.A.at[q, i, j] if ph == 0 else self.B.at[q, j, i]

        send, recv = self.xsend.at[ph, q, j, kind], self.xrecv.at[ph, q, j, kind]
        up, down = self.at(1, 0), self.at(NX - 1, 0)
        if kind == 0:
            return remote(self.Q.at[ph, q, j, 0], place(3), send, recv, up)
        if kind == 1:
            return remote(self.Q.at[ph, q, j, 1], place(1), send, recv, down)
        h = kind % 2
        half = place(2).at[:, pl.ds(h * self.piece, self.piece)]
        where = down if h else up
        if kind >= 4:
            return remote(self.TR.at[ph, q, j, h], half, send, recv, where)
        if j == FAR:
            return remote(self.QH.at[ph, q, j, h], half, send, recv, self.at(2, 0))
        return remote(self.QH.at[ph, q, j, h], self.TR.at[ph, q, j, h], send, recv, where)

    def send_buckets(self, ph, q, j, rows):
        n = BUCKET
        for h in range(2):
            self.QH[ph, q, j, h] = rows[2 * n : 3 * n, h * self.piece : (h + 1) * self.piece]
            self.bucket(ph, q, j, 2 + h).start()
        self.Q[ph, q, j, 0] = rows[n : 2 * n]
        self.bucket(ph, q, j, 0).start()
        self.Q[ph, q, j, 1] = rows[3 * n :]
        self.bucket(ph, q, j, 1).start()
        if ph == 0:
            self.A[q, 0, j] = rows[:n]
        else:
            self.B[q, j, 0] = rows[:n]

    def relay(self, ph, q, *js):
        for j in js:
            if j != FAR:
                for h in range(2):
                    self.bucket(ph, q, j, 2 + h).wait_recv()
                    self.bucket(ph, q, j, 4 + h).start()

    def landed(self, ph, q, j):
        for kind in (0, 1, 2, 3) if j == FAR else (0, 1, 4, 5):
            self.bucket(ph, q, j, kind).wait_recv()

    def row_codes(self, shape, dim):
        line = lax.broadcasted_iota(I32, shape, dim)
        dx = sum((line >= BUCKET * k).astype(I32) for k in (1, 2, 3))
        owner = ((self.x + dx) % NX) * NZ + self.z
        return jnp.where(line < BUCKET * NX, owner * BUCKET + line - BUCKET * dx, -7)

    def select(self, q, *js):
        for j in js:
            rows = self.row_codes((NX * BUCKET, self.C.shape[2]), 0)
            hit = onehot((rows == self.C[j, 0:1]) | (rows == self.C[j, 1:2]))
            parts = [dot(hit, self.G[j, 2 * q + h]) for h in range(2)]
            self.send_buckets(0, q, j, jnp.concatenate(parts, axis=1).astype(BF16))

    def normalize(self, tokens, gain):
        values = tokens[...].astype(F32)
        scale = lax.rsqrt(jnp.mean(values * values, axis=-1, keepdims=True) + EPSILON)
        normed = (values * scale * gain[...]).astype(BF16)
        for p in range(4):
            self.G[0, p] = normed[:, p * self.piece : (p + 1) * self.piece]

    def open_ring(self, *ps):
        for p in ps:
            self.spread(1, p, True).start()
            self.spread(NZ - 1, p, False).start()

    def hop(self, s, *ps):
        for p in ps:
            for up in (True, False):
                j, onward = (s, s + 1) if up else (NZ - s, NZ - s - 1)
                far_way = up == (p % 2 == 0)
                if s < FAR or far_way:
                    self.spread(j, p, up).wait_recv()
                if s < FAR - 1 or (s == FAR - 1 and far_way):
                    self.spread(onward, p, up).start()

    def compact(self, q, rows):
        for j in range(NZ):
            self.landed(0, q, j)
        _, experts, cap, width = rows.shape
        total = NX * NZ * BUCKET
        arrived = self.A[q].reshape(total, width)
        per = experts // 2
        for b in range(2):
            places = down_rows(self.PO[b : b + 1])[:, :1]
            hit = onehot(places == lax.broadcasted_iota(I32, (per * cap, total), 1))
            got = dot(hit, arrived).astype(BF16)
            for i in range(per):
                rows[q, b * per + i] = got[i * cap : (i + 1) * cap]

    def expanders(self):
        n = self.C.shape[2]
        codes = self.row_codes((n, 128), 1)
        for j in range(NZ):
            first, second = down_rows(self.C[j, 0:1]), down_rows(self.C[j, 1:2])
            self.OT[j] = onehot((first == codes) | (second == codes))

    def send_back(self, q, weighted, *js):
        _, experts, cap, width = weighted.shape
        per = experts // 2
        line = lax.broadcasted_iota(I32, (NX * BUCKET, per * cap), 0)
        dx = sum((line >= BUCKET * k).astype(I32) for k in (1, 2, 3))
        base = dx * (NZ * BUCKET) + line - BUCKET * dx
        for j in js:
            out = 0
            for b in range(2):
                hit = onehot(base + j * BUCKET == self.PO[b : b + 1])
                out = out + dot(hit, weighted[q, b * per : (b + 1) * per].reshape(per * cap, width))
            self.send_buckets(1, q, j, out.astype(BF16))

    def part(self, j, p):
        q, h = p // 2, p % 2
        n = NX * BUCKET
        rows = self.B[q, j, :, :, h * self.piece : (h + 1) * self.piece].reshape(n, self.piece)
        return dot(self.OT[j][:, :n], rows)

    def fold(self, j, p, up):
        where, way = (self.at(0, 1), 0) if up else (self.at(0, NZ - 1), 1)
        there = (j + 1) % NZ if up else j - 1
        return remote(
            self.V.at[j, p], self.RP.at[way, there, p], self.vsend.at[j, p], self.vrecv.at[way, there, p], where
        )

    def carried(self, j, p, up):
        self.fold((j - 1) % NZ if up else j + 1, p, up).wait_recv()
        return self.RP[0 if up else 1, j, p].astype(F32)

    def emit(self, j, p, up, incoming):
        value = self.part(j, p)
        if incoming:
            value = value + self.carried(j, p, up)
        self.V[j, p] = value.astype(BF16)
        self.fold(j, p, up).start()

    def fold_far(self, q):
        self.landed(1, q, FAR)
        self.emit(FAR, 2 * q, True, False)
        self.emit(FAR, 2 * q + 1, False, False)

    def fold_step(self, q, s):
        up, down = FAR + s, FAR - s
        even, odd = 2 * q, 2 * q + 1
        for j in (up, down):
            self.landed(1, q, j)
        self.emit(up, odd, True, s > 1)
        self.emit(down, even, False, s > 1)
        self.emit(up, even, True, True)
        self.emit(down, odd, False, True)

    def fold_end(self, q, tokens, out):
        self.landed(1, q, 0)
        for p in (2 * q, 2 * q + 1):
            cut = slice(p * self.piece, (p + 1) * self.piece)
            total = tokens[:, cut].astype(F32) + self.part(0, p)
            total = total + self.carried(0, p, True) + self.carried(0, p, False)
            out[:, cut] = total.astype(BF16)

    def drain(self, ph):
        for q in range(2):
            for j in range(NZ):
                for kind in range(4 if j == FAR else 6):
                    self.bucket(ph, q, j, kind).wait_send()
        for j in range(1, NZ):
            if ph == 0:
                self.code(j).wait_send()
            for p in range(4):
                far_up = j == FAR and p % 2 == 0
                if ph == 0:
                    self.spread(j, p, j < FAR or far_up).wait_send()
                else:
                    self.fold(j, p, j > FAR or far_up).wait_send()

    @staticmethod
    def scratch(tok_rows, width, slots):
        dma = pltpu.SemaphoreType.DMA
        chunk, piece = width // 2, width // 4
        return dict(
            G=pltpu.VMEM((NZ, 4, tok_rows, piece), BF16),
            C=pltpu.VMEM((NZ, 2, tok_rows), I32),
            PO=pltpu.VMEM((2, slots // 2), I32),
            Q=pltpu.VMEM((2, 2, NZ, 2, BUCKET, chunk), BF16),
            QH=pltpu.VMEM((2, 2, NZ, 2, BUCKET, piece), BF16),
            TR=pltpu.VMEM((2, 2, NZ, 2, BUCKET, piece), BF16),
            A=pltpu.VMEM((2, NX, NZ, BUCKET, chunk), BF16),
            B=pltpu.VMEM((2, NZ, NX, BUCKET, chunk), BF16),
            OT=pltpu.VMEM((NZ, tok_rows, 128), BF16),
            V=pltpu.VMEM((NZ, 4, tok_rows, piece), BF16),
            RP=pltpu.VMEM((2, NZ, 4, tok_rows, piece), BF16),
            gsend=dma((NZ, 4)),
            grecv=dma((NZ, 4)),
            csend=dma((NZ,)),
            crecv=dma((NZ,)),
            xsend=dma((2, 2, NZ, 6)),
            xrecv=dma((2, 2, NZ, 6)),
            vsend=dma((NZ, 4)),
            vrecv=dma((2, NZ, 4)),
        )


class Experts:
    def __init__(self, refs, rows, router, w1_hbm, w2_hbm):
        self.__dict__.update(refs)
        self.rows, self.router, self.w1_hbm, self.w2_hbm = rows, router, w1_hbm, w2_hbm
        _, self.experts, self.cap, self.chunk = rows.shape
        self.half = self.experts // 2
        dat = lax.axis_index("dat")
        c, y = dat % 2, dat // 2
        self.partner = {"dat": y * 2 + 1 - c}
        self.plus = {"dat": ((y + 1) % NY) * 2 + c}
        self.minus = {"dat": ((y + NY - 1) % NY) * 2 + c}
        self.own, self.other = pl.ds(0, self.cap), pl.ds(self.cap, self.cap)

    def peers(self):
        return [self.partner, self.plus, self.minus]

    def weights(self, e):
        return [
            pltpu.make_async_copy(self.w1_hbm.at[e], self.W1.at[e], self.w_sem.at[0, e]),
            pltpu.make_async_copy(self.w2_hbm.at[e], self.W2.at[e], self.w_sem.at[1, e]),
        ]

    def load(self):
        for e in range(self.experts):
            for copy in self.weights(e):
                copy.start()

    def direct(self, q, s, e):
        return remote(
            self.rows.at[q, e], self.X.at[q, e, s, self.own], self.sendI.at[q, s, e], self.recvI.at[q, s, e],
            self.plus if s == 1 else self.minus,
        )

    def onward(self, q, e):
        s, where = (1, self.plus) if e < self.half else (2, self.minus)
        return remote(
            self.X.at[q, e, s, self.own], self.X.at[q, e, 3, self.own],
            self.sendI.at[q, 3, e], self.recvI.at[q, 3, e], where,
        )

    def across(self, q, s, e, own=False):
        src = self.rows.at[q, e] if own else self.X.at[q, e, s, self.own]
        return remote(
            src, self.X.at[q, e, s, self.other], self.sendP.at[q, s, e], self.recvP.at[q, s, e], self.partner
        )

    def part_across(self, q, s, e):
        return remote(
            self.PS.at[q, e, s, self.other], self.R.at[q, e, s],
            self.rsend.at[q, s, e], self.rrecv.at[q, s, e], self.partner,
        )

    def final(self, q, up, e):
        src, i, where = (self.S.at[q, e, 2], 0, self.plus) if up else (self.S.at[q, e, 1], 1, self.minus)
        return remote(src, self.F.at[q, i, e], self.fsend.at[q, i, e], self.frecv.at[q, i, e], where)

    def transit(self, q, e):
        where = self.plus if e < self.half else self.minus
        return remote(self.S.at[q, e, 3], self.T.at[q, e], self.tsend.at[q, e], self.trecv.at[q, e], where)

    def pairs(self, k):
        experts, half = self.experts, self.half
        if k < experts:
            return [(1, k), (2, (k + half) % experts)]
        if k < experts + half:
            return [(3, k - experts), (3, k - experts + half)]
        return []

    def begin(self, q):
        for e in range(self.experts):
            self.across(q, 0, e, True).start()
        for k in range(self.experts):
            for s, e in self.pairs(k):
                self.direct(q, s, e).start()
        for e in range(self.experts):
            self.X[q, e, 0, : self.cap] = self.rows[q, e]

    def receive(self, q, *ks):
        for k in ks:
            for s, e in self.pairs(k):
                copy = self.onward(q, e) if s == 3 else self.direct(q, s, e)
                copy.wait_recv()
                self.across(q, s, e).start()
                if k < self.half:
                    self.onward(q, e).start()

    def matmuls(self, e, s, n):
        chunk, tall = self.chunk, n * 2 * self.cap
        inner = 0.0
        for q in range(2):
            block = self.X[q, e, s : s + n].reshape(tall, chunk)
            inner = inner + dot(block, self.W1[e, q * chunk : (q + 1) * chunk])
        hidden = jnp.maximum(inner, 0.0).astype(BF16)
        for q in range(2):
            sums = dot(hidden, self.W2[e, :, q * chunk : (q + 1) * chunk]).astype(BF16)
            self.PS[q, e, s : s + n] = sums.reshape(n, 2 * self.cap, chunk)

    def local(self):
        def one(e, carry):
            for copy in self.weights(e):
                copy.wait()
            for q in range(2):
                self.across(q, 0, e, True).wait_recv()
            self.matmuls(e, 0, 1)
            for q in range(2):
                self.part_across(q, 0, e).start()
            return carry

        lax.fori_loop(0, self.experts, one, 0)

    def compute(self, s, n, *es):
        for e in es:
            for i in range(n):
                for q in range(2):
                    self.across(q, s + i, e).wait_recv()
        first, gap = es[0], es[1] - es[0]

        def one(i, carry):
            self.matmuls(first + gap * i, s, n)
            return carry

        lax.fori_loop(0, 2, one, 0)
        for q in range(2):
            for e in es:
                for i in range(n):
                    self.part_across(q, s + i, e).start()

    def chip_sum(self, q, s, e):
        self.part_across(q, s, e).wait_recv()
        return self.PS[q, e, s, : self.cap].astype(F32) + self.R[q, e, s].astype(F32)

    def settle(self, s, n, *es):
        for q in range(2):
            self.settle_chunk(q, s, n, *es)

    def settle_chunk(self, q, s, n, *es):
        for e in es:
            for i in range(n):
                self.S[q, e, s + i] = self.chip_sum(q, s + i, e).astype(BF16)
                if s == 3:
                    self.transit(q, e).start()
                elif (s + i == 1) == (e < self.half):
                    self.final(q, s + i == 2, e).start()

    def pass_on(self, q):
        for k in range(self.half):
            for e, s in ((k, 2), (k + self.half, 1)):
                self.transit(q, e).wait_recv()
                self.S[q, e, s] = (self.S[q, e, s].astype(F32) + self.T[q, e].astype(F32)).astype(BF16)
                self.final(q, s == 2, e).start()

    def gates(self):
        chunk = self.chunk
        for e in range(self.experts):
            logits = 0.0
            for q in range(2):
                weight = self.router[e : e + 1, q * chunk : (q + 1) * chunk].astype(F32)
                logits = logits + jnp.sum(self.rows[q, e].astype(F32) * weight, axis=1, keepdims=True)
            self.GT[e] = jax.nn.sigmoid(logits)

    def finish(self, q, weighted):
        for e in range(self.experts):
            total = self.chip_sum(q, 0, e)
            for up in (True, False):
                self.final(q, up, e).wait_recv()
            total = total + self.F[q, 0, e].astype(F32) + self.F[q, 1, e].astype(F32)
            weighted[q, e] = (self.GT[e] * total).astype(BF16)

    def run(self):
        half = self.half
        early, late = range(0, self.experts, half), range(1, self.experts, half)
        self.local()
        self.receive(0, *range(2 * half, 3 * half))
        self.receive(1, *range(half + 1))
        self.compute(1, 2, *early)
        self.receive(1, half + 1)
        self.compute(1, 2, *late)
        self.settle(1, 2, *early)
        self.receive(1, *range(2 * half, 3 * half))
        self.compute(3, 1, *early)
        self.settle(1, 2, *late)
        self.compute(3, 1, *late)
        for q in range(2):
            self.settle_chunk(q, 3, 1, *early, *late)
        for q in range(2):
            self.pass_on(q)

    def drain(self):
        for q in range(2):
            for e in range(self.experts):
                self.direct(q, 1, e).wait_send()
                self.direct(q, 2, e).wait_send()
                self.onward(q, e).wait_send()
                self.final(q, True, e).wait_send()
                self.final(q, False, e).wait_send()
                self.transit(q, e).wait_send()
                for s in range(4):
                    self.across(q, s, e, s == 0).wait_send()
                    self.part_across(q, s, e).wait_send()

    @staticmethod
    def scratch(experts, cap, width, hidden):
        dma = pltpu.SemaphoreType.DMA
        chunk = width // 2
        return dict(
            X=pltpu.VMEM((2, experts, 4, 2 * cap, chunk), BF16),
            W1=pltpu.VMEM((experts, width, hidden), BF16),
            W2=pltpu.VMEM((experts, hidden, width), BF16),
            PS=pltpu.VMEM((2, experts, 4, 2 * cap, chunk), BF16),
            R=pltpu.VMEM((2, experts, 4, cap, chunk), BF16),
            S=pltpu.VMEM((2, experts, 4, cap, chunk), BF16),
            T=pltpu.VMEM((2, experts, cap, chunk), BF16),
            F=pltpu.VMEM((2, 2, experts, cap, chunk), BF16),
            GT=pltpu.VMEM((experts, cap, 1), F32),
            w_sem=dma((2, experts)),
            sendP=dma((2, 4, experts)),
            recvP=dma((2, 4, experts)),
            sendI=dma((2, 4, experts)),
            recvI=dma((2, 4, experts)),
            rsend=dma((2, 4, experts)),
            rrecv=dma((2, 4, experts)),
            fsend=dma((2, 2, experts)),
            frecv=dma((2, 2, experts)),
            tsend=dma((2, experts)),
            trecv=dma((2, experts)),
        )


class NoExperts:
    def __init__(self, rows):
        self.rows = rows

    def __getattr__(self, name):
        return lambda *_: []

    def finish(self, q, weighted):
        for e in range(self.rows.shape[1]):
            weighted[q, e] = self.rows[q, e]


def layer_kernel(
    names, with_experts, dat_count, tokens, gain, ids, picks, router, w1_hbm, w2_hbm, out, rows, weighted, *refs
):
    refs = dict(zip(names, refs))
    tok_rows, width = tokens.shape
    ex = Exchange({k: refs.pop(k) for k in Exchange.scratch(8, 8, 8)}, width)
    xp = Experts(refs, rows, router, w1_hbm, w2_hbm) if with_experts else NoExperts(rows)
    xp.load()
    barrier = pltpu.get_barrier_semaphore()
    others = ex.peers() + xp.peers()
    for other in others:
        pl.semaphore_signal(barrier, inc=1, device_id=other, device_id_type=MESH)
    ex.routes(ids, picks, tok_rows, picks.shape[0] * picks.shape[1], dat_count)
    ex.normalize(tokens, gain)
    pl.semaphore_wait(barrier, len(others))

    ex.open_codes()
    ex.open_ring(0, 1, 2)
    ex.select(0, 0)
    ex.code_hop(1)
    ex.hop(1, 0, 1)
    ex.open_ring(3)
    ex.select(0, 1, 7)
    ex.code_hop(2)
    ex.hop(2, 0, 1)
    ex.hop(1, 2)
    ex.relay(0, 0, 0)
    ex.select(0, 2, 6)
    ex.select(1, 0)
    ex.code_hop(3)
    ex.hop(3, 0, 1)
    ex.hop(1, 3)
    ex.relay(0, 0, 1, 7)
    ex.select(0, 3, 5)
    ex.select(1, 1, 7)
    ex.code_hop(4)
    ex.hop(4, 0, 1)
    ex.select(0, 4)
    ex.hop(2, 2, 3)
    ex.relay(0, 0, 2, 6)
    ex.relay(0, 0, 3, 5)
    ex.relay(0, 1, 0)
    ex.select(1, 2, 6)
    ex.relay(0, 1, 1, 7)
    ex.hop(3, 2, 3)
    ex.select(1, 3, 5)
    ex.compact(0, rows)
    xp.begin(0)
    ex.relay(0, 1, 2, 6)
    ex.hop(4, 2, 3)
    ex.select(1, 4)
    ex.relay(0, 1, 3, 5)
    xp.receive(0, 0, 1)
    ex.compact(1, rows)
    xp.begin(1)
    xp.receive(0, 2, 3)
    xp.gates()
    ex.expanders()
    xp.run()

    steps = [(s, q, js) for s, js in ((1, (5, 3)), (2, (6, 2)), (3, (7, 1)), (4, (0,))) for q in range(2)]

    def send_ahead(h):
        if h < len(steps):
            _, q, js = steps[h]
            ex.send_back(q, weighted, *js)

    xp.finish(0, weighted)
    ex.send_back(0, weighted, FAR)
    send_ahead(0)
    xp.finish(1, weighted)
    ex.send_back(1, weighted, FAR)
    send_ahead(1)
    ex.fold_far(0)
    ex.relay(1, 0, *steps[0][2])
    ex.fold_far(1)
    send_ahead(2)
    ex.drain(0)
    for h, (s, q, js) in enumerate(steps):
        if h + 1 < len(steps):
            ex.relay(1, steps[h + 1][1], *steps[h + 1][2])
        send_ahead(h + 3)
        if s < FAR:
            ex.fold_step(q, s)
        else:
            if q == 0:
                xp.drain()
            ex.fold_end(q, tokens, out)
    ex.drain(1)


def whole_layer(tokens, gain, ids, picks, router, inner_weight, outer_weight, dat_count, with_experts=True):
    tok_rows, width = tokens.shape
    experts, _, hidden = inner_weight.shape
    cap = picks.shape[1]
    vmem = pl.BlockSpec(memory_space=pltpu.VMEM)
    hbm = pl.BlockSpec(memory_space=pl.ANY)
    scratch = Exchange.scratch(tok_rows, width, experts * cap)
    if with_experts:
        scratch.update(Experts.scratch(experts, cap, width, hidden))
    slots = pltpu.VMEM((2, experts, cap, width // 2), BF16)
    return pl.pallas_call(
        functools.partial(layer_kernel, tuple(scratch), with_experts, dat_count),
        name="whole_layer",
        out_shape=jax.ShapeDtypeStruct((tok_rows, width), BF16),
        in_specs=[vmem] * 5 + [hbm] * 2,
        out_specs=vmem,
        scratch_shapes=[slots, slots] + list(scratch.values()),
        compiler_params=pltpu.CompilerParams(
            collective_id=0, has_side_effects=True, vmem_limit_bytes=60 * 1024 * 1024
        ),
    )(tokens, gain, ids, picks, router, inner_weight, outer_weight)


def body(tokens, norm_gain, router_weight, inner_weight, outer_weight, slot_tokens, slot_ids):
    return whole_layer(
        tokens, norm_gain[None, :], slot_ids.T, slot_tokens, router_weight.T, inner_weight, outer_weight,
        lax.axis_size("dat"),
    )


def solution(mesh):
    in_specs = (
        P(("exp", "dat"), None),
        P(),
        P(None, "exp"),
        P("exp", None, "dat"),
        P("exp", "dat", None),
        P("exp", "dat"),
        P(("exp", "dat"), None),
    )
    out_specs = P(("exp", "dat"), None)
    return jax.shard_map(body, mesh=mesh, in_specs=in_specs, out_specs=out_specs, check_vma=False)
```

```python
import functools

import jax
import jax.numpy as jnp
from jax import lax
from jax.experimental import pallas as pl
from jax.experimental.pallas import tpu as pltpu
from jax.sharding import PartitionSpec as P

EPSILON = 1e-06
MESH = pl.DeviceIdType.MESH
BF16 = jnp.bfloat16
F32 = jnp.float32
I32 = jnp.int32

NX, NZ, NY = 4, 8, 4
BUCKET = 24
FAR = NZ // 2
NP = 8


def dot(a, b):
    return jnp.dot(a, b, preferred_element_type=F32)


def onehot(mask):
    return mask.astype(F32).astype(BF16)


def down_rows(row):
    n = row.shape[1]
    return jnp.transpose(jnp.broadcast_to(row, (n, n)))


def count(mask):
    return jnp.sum(mask.astype(F32), axis=0, keepdims=True).astype(I32)


def remote(src, dst, send, recv, where):
    return pltpu.make_async_remote_copy(
        src_ref=src, dst_ref=dst, send_sem=send, recv_sem=recv, device_id=where, device_id_type=MESH
    )


def pieces(q):
    return list(range(q * NP // 2, (q + 1) * NP // 2))


class Exchange:
    def __init__(self, refs, width):
        self.__dict__.update(refs)
        exp = lax.axis_index("exp")
        self.x, self.z = exp // NZ, exp % NZ
        self.chunk, self.piece = width // 2, width // NP

    def at(self, dx, dz):
        return {"exp": ((self.x + dx) % NX) * NZ + (self.z + dz) % NZ}

    def peers(self):
        return [self.at(0, 1), self.at(0, NZ - 1)] + [self.at(dx, 0) for dx in range(1, NX)]

    def routes(self, slot_ids, slot_tokens, tok_rows, slots, dat_count):
        ids = [slot_ids[k : k + 1] for k in range(2)]
        owners = [row // (slots * dat_count) for row in ids]
        for k in range(2):
            rank = 0
            for m in range(2):
                rank = rank + count((down_rows(owners[m]) == owners[k]) & (down_rows(ids[m]) < ids[k]))
            self.C[0, k : k + 1] = owners[k] * BUCKET + rank
        experts = slot_tokens.shape[0]
        per = experts // 2
        source = [
            jnp.concatenate([slot_tokens[b * per + i : b * per + i + 1] for i in range(per)], axis=1)
            // (tok_rows * dat_count)
            for b in range(2)
        ]
        n = slots // 2
        earlier = lax.broadcasted_iota(I32, (n, n), 0) < lax.broadcasted_iota(I32, (n, n), 1)
        for b in range(2):
            rank = count((down_rows(source[b]) == source[b]) & earlier)
            if b == 1:
                rank = rank + count(down_rows(source[0]) == source[1])
            place = ((source[b] // NZ - self.x + NX) % NX) * NZ + (self.z - source[b] % NZ + NZ) % NZ
            self.PO[b : b + 1] = place * BUCKET + rank

    def spread(self, j, p, up):
        src = self.G.at[(j - 1) if up else (j + 1) % NZ, p]
        where = self.at(0, 1) if up else self.at(0, NZ - 1)
        return remote(src, self.G.at[j, p], self.gsend.at[j, p], self.grecv.at[j, p], where)

    def code(self, j):
        up = j <= FAR
        src = self.C.at[(j - 1) if up else (j + 1) % NZ]
        where = self.at(0, 1) if up else self.at(0, NZ - 1)
        return remote(src, self.C.at[j], self.csend.at[j], self.crecv.at[j], where)

    def open_codes(self):
        self.code(1).start()
        self.code(NZ - 1).start()

    def code_hop(self, s):
        self.code(s).wait_recv()
        if s < FAR:
            self.code(s + 1).start()
            self.code(NZ - s).wait_recv()
            if s < FAR - 1:
                self.code(NZ - s - 1).start()

    def bucket(self, ph, q, j, dx):
        there = NX - dx
        dst = self.A.at[q, there, j] if ph == 0 else self.B.at[q, j, there]
        i = dx - 1
        return remote(
            self.Q.at[ph, q, j, i], dst, self.xsend.at[ph, q, j, i], self.xrecv.at[ph, q, j, i], self.at(dx, 0)
        )

    def send_buckets(self, ph, q, j, rows):
        n = BUCKET
        for dx in (2, 1, 3):
            self.Q[ph, q, j, dx - 1] = rows[dx * n : (dx + 1) * n]
            self.bucket(ph, q, j, dx).start()
        if ph == 0:
            self.A[q, 0, j] = rows[:n]
        else:
            self.B[q, j, 0] = rows[:n]

    def landed(self, ph, q, j):
        for dx in range(1, NX):
            self.bucket(ph, q, j, dx).wait_recv()

    def row_codes(self, shape, dim):
        line = lax.broadcasted_iota(I32, shape, dim)
        dx = sum((line >= BUCKET * k).astype(I32) for k in (1, 2, 3))
        owner = ((self.x + dx) % NX) * NZ + self.z
        return jnp.where(line < BUCKET * NX, owner * BUCKET + line - BUCKET * dx, -7)

    def select(self, q, *js):
        for j in js:
            rows = self.row_codes((NX * BUCKET, self.C.shape[2]), 0)
            hit = onehot((rows == self.C[j, 0:1]) | (rows == self.C[j, 1:2]))
            parts = [dot(hit, self.G[j, p]) for p in pieces(q)]
            self.send_buckets(0, q, j, jnp.concatenate(parts, axis=1).astype(BF16))

    def normalize(self, tokens, gain):
        values = tokens[...].astype(F32)
        scale = lax.rsqrt(jnp.mean(values * values, axis=-1, keepdims=True) + EPSILON)
        normed = (values * scale * gain[...]).astype(BF16)
        for p in range(NP):
            self.G[0, p] = normed[:, p * self.piece : (p + 1) * self.piece]

    def open_ring(self, *ps):
        for p in ps:
            self.spread(1, p, True).start()
            self.spread(NZ - 1, p, False).start()

    def hop(self, s, *ps):
        for p in ps:
            for up in (True, False):
                j, onward = (s, s + 1) if up else (NZ - s, NZ - s - 1)
                far_way = up == (p % 2 == 0)
                if s < FAR or far_way:
                    self.spread(j, p, up).wait_recv()
                if s < FAR - 1 or (s == FAR - 1 and far_way):
                    self.spread(onward, p, up).start()

    def compact(self, q, rows):
        for j in range(NZ):
            self.landed(0, q, j)
        _, experts, cap, width = rows.shape
        total = NX * NZ * BUCKET
        arrived = self.A[q].reshape(total, width)
        per = experts // 2
        for b in range(2):
            places = down_rows(self.PO[b : b + 1])[:, :1]
            hit = onehot(places == lax.broadcasted_iota(I32, (per * cap, total), 1))
            got = dot(hit, arrived).astype(BF16)
            for i in range(per):
                rows[q, b * per + i] = got[i * cap : (i + 1) * cap]

    def expanders(self):
        n = self.C.shape[2]
        codes = self.row_codes((n, 128), 1)
        for j in range(NZ):
            first, second = down_rows(self.C[j, 0:1]), down_rows(self.C[j, 1:2])
            self.OT[j] = onehot((first == codes) | (second == codes))

    def send_back(self, q, weighted, *js):
        _, experts, cap, width = weighted.shape
        per = experts // 2
        line = lax.broadcasted_iota(I32, (NX * BUCKET, per * cap), 0)
        dx = sum((line >= BUCKET * k).astype(I32) for k in (1, 2, 3))
        base = dx * (NZ * BUCKET) + line - BUCKET * dx
        for j in js:
            out = 0
            for b in range(2):
                hit = onehot(base + j * BUCKET == self.PO[b : b + 1])
                out = out + dot(hit, weighted[q, b * per : (b + 1) * per].reshape(per * cap, width))
            self.send_buckets(1, q, j, out.astype(BF16))

    def part(self, j, p):
        q, h = p // (NP // 2), p % (NP // 2)
        n = NX * BUCKET
        rows = self.B[q, j, :, :, h * self.piece : (h + 1) * self.piece].reshape(n, self.piece)
        return dot(self.OT[j][:, :n], rows)

    def fold(self, j, p, up):
        where, way = (self.at(0, 1), 0) if up else (self.at(0, NZ - 1), 1)
        there = (j + 1) % NZ if up else j - 1
        return remote(
            self.V.at[j, p], self.RP.at[way, there, p], self.vsend.at[j, p], self.vrecv.at[way, there, p], where
        )

    def carried(self, j, p, up):
        self.fold((j - 1) % NZ if up else j + 1, p, up).wait_recv()
        return self.RP[0 if up else 1, j, p].astype(F32)

    def emit(self, j, p, up, incoming):
        value = self.part(j, p)
        if incoming:
            value = value + self.carried(j, p, up)
        self.V[j, p] = value.astype(BF16)
        self.fold(j, p, up).start()

    def fold_far(self, q):
        self.landed(1, q, FAR)
        for p in pieces(q):
            self.emit(FAR, p, p % 2 == 0, False)

    def fold_step(self, q, s):
        up, down = FAR + s, FAR - s
        for j in (up, down):
            self.landed(1, q, j)
        for first in (True, False):
            for p in pieces(q):
                rising = (p % 2 == 1) == first
                self.emit(up if rising else down, p, rising, s > 1 or not first)

    def fold_end(self, q, tokens, out):
        self.landed(1, q, 0)
        for p in pieces(q):
            cut = slice(p * self.piece, (p + 1) * self.piece)
            total = tokens[:, cut].astype(F32) + self.part(0, p)
            total = total + self.carried(0, p, True) + self.carried(0, p, False)
            out[:, cut] = total.astype(BF16)

    def drain(self, ph):
        for q in range(2):
            for j in range(NZ):
                for dx in range(1, NX):
                    self.bucket(ph, q, j, dx).wait_send()
        for j in range(1, NZ):
            if ph == 0:
                self.code(j).wait_send()
            for p in range(NP):
                far_up = j == FAR and p % 2 == 0
                if ph == 0:
                    self.spread(j, p, j < FAR or far_up).wait_send()
                else:
                    self.fold(j, p, j > FAR or far_up).wait_send()

    @staticmethod
    def scratch(tok_rows, width, slots):
        dma = pltpu.SemaphoreType.DMA
        chunk, piece = width // 2, width // NP
        return dict(
            G=pltpu.VMEM((NZ, NP, tok_rows, piece), BF16),
            C=pltpu.VMEM((NZ, 2, tok_rows), I32),
            PO=pltpu.VMEM((2, slots // 2), I32),
            Q=pltpu.VMEM((2, 2, NZ, NX - 1, BUCKET, chunk), BF16),
            A=pltpu.VMEM((2, NX, NZ, BUCKET, chunk), BF16),
            B=pltpu.VMEM((2, NZ, NX, BUCKET, chunk), BF16),
            OT=pltpu.VMEM((NZ, tok_rows, 128), BF16),
            V=pltpu.VMEM((NZ, NP, tok_rows, piece), BF16),
            RP=pltpu.VMEM((2, NZ, NP, tok_rows, piece), BF16),
            gsend=dma((NZ, NP)),
            grecv=dma((NZ, NP)),
            csend=dma((NZ,)),
            crecv=dma((NZ,)),
            xsend=dma((2, 2, NZ, NX - 1)),
            xrecv=dma((2, 2, NZ, NX - 1)),
            vsend=dma((NZ, NP)),
            vrecv=dma((2, NZ, NP)),
        )


class Experts:
    def __init__(self, refs, rows, router, w1_hbm, w2_hbm):
        self.__dict__.update(refs)
        self.rows, self.router, self.w1_hbm, self.w2_hbm = rows, router, w1_hbm, w2_hbm
        _, self.experts, self.cap, self.chunk = rows.shape
        self.half = self.experts // 2
        dat = lax.axis_index("dat")
        c, y = dat % 2, dat // 2
        self.partner = {"dat": y * 2 + 1 - c}
        self.plus = {"dat": ((y + 1) % NY) * 2 + c}
        self.minus = {"dat": ((y + NY - 1) % NY) * 2 + c}
        self.own, self.other = pl.ds(0, self.cap), pl.ds(self.cap, self.cap)

    def peers(self):
        return [self.partner, self.plus, self.minus]

    def weights(self, e):
        return [
            pltpu.make_async_copy(self.w1_hbm.at[e], self.W1.at[e], self.w_sem.at[0, e]),
            pltpu.make_async_copy(self.w2_hbm.at[e], self.W2.at[e], self.w_sem.at[1, e]),
        ]

    def load(self):
        for e in range(self.experts):
            for copy in self.weights(e):
                copy.start()

    def direct(self, q, s, e):
        return remote(
            self.rows.at[q, e], self.X.at[q, e, s, self.own], self.sendI.at[q, s, e], self.recvI.at[q, s, e],
            self.plus if s == 1 else self.minus,
        )

    def onward(self, q, e):
        s, where = (1, self.plus) if e < self.half else (2, self.minus)
        return remote(
            self.X.at[q, e, s, self.own], self.X.at[q, e, 3, self.own],
            self.sendI.at[q, 3, e], self.recvI.at[q, 3, e], where,
        )

    def across(self, q, s, e, own=False):
        src = self.rows.at[q, e] if own else self.X.at[q, e, s, self.own]
        return remote(
            src, self.X.at[q, e, s, self.other], self.sendP.at[q, s, e], self.recvP.at[q, s, e], self.partner
        )

    def part_across(self, q, s, e):
        return remote(
            self.PS.at[q, e, s, self.other], self.R.at[q, e, s],
            self.rsend.at[q, s, e], self.rrecv.at[q, s, e], self.partner,
        )

    def final(self, q, up, e):
        src, i, where = (self.S.at[q, e, 2], 0, self.plus) if up else (self.S.at[q, e, 1], 1, self.minus)
        return remote(src, self.F.at[q, i, e], self.fsend.at[q, i, e], self.frecv.at[q, i, e], where)

    def transit(self, q, e):
        where = self.plus if e < self.half else self.minus
        return remote(self.S.at[q, e, 3], self.T.at[q, e], self.tsend.at[q, e], self.trecv.at[q, e], where)

    def pairs(self, k):
        experts, half = self.experts, self.half
        if k < experts:
            return [(1, k), (2, (k + half) % experts)]
        if k < experts + half:
            return [(3, k - experts), (3, k - experts + half)]
        return []

    def begin(self, q):
        for e in range(self.experts):
            self.across(q, 0, e, True).start()
        for k in range(self.experts):
            for s, e in self.pairs(k):
                self.direct(q, s, e).start()
        for e in range(self.experts):
            self.X[q, e, 0, : self.cap] = self.rows[q, e]

    def receive(self, q, *ks):
        for k in ks:
            for s, e in self.pairs(k):
                copy = self.onward(q, e) if s == 3 else self.direct(q, s, e)
                copy.wait_recv()
                self.across(q, s, e).start()
                if k < self.half:
                    self.onward(q, e).start()

    def matmuls(self, e, s, n):
        chunk, tall = self.chunk, n * 2 * self.cap
        inner = 0.0
        for q in range(2):
            block = self.X[q, e, s : s + n].reshape(tall, chunk)
            inner = inner + dot(block, self.W1[e, q * chunk : (q + 1) * chunk])
        hidden = jnp.maximum(inner, 0.0).astype(BF16)
        for q in range(2):
            sums = dot(hidden, self.W2[e, :, q * chunk : (q + 1) * chunk]).astype(BF16)
            self.PS[q, e, s : s + n] = sums.reshape(n, 2 * self.cap, chunk)

    def local(self):
        def one(e, carry):
            for copy in self.weights(e):
                copy.wait()
            for q in range(2):
                self.across(q, 0, e, True).wait_recv()
            self.matmuls(e, 0, 1)
            for q in range(2):
                self.part_across(q, 0, e).start()
            return carry

        lax.fori_loop(0, self.experts, one, 0)

    def compute(self, s, n, *es):
        for e in es:
            for i in range(n):
                for q in range(2):
                    self.across(q, s + i, e).wait_recv()
        first, gap = es[0], es[1] - es[0]

        def one(i, carry):
            self.matmuls(first + gap * i, s, n)
            return carry

        lax.fori_loop(0, 2, one, 0)
        for q in range(2):
            for e in es:
                for i in range(n):
                    self.part_across(q, s + i, e).start()

    def chip_sum(self, q, s, e):
        self.part_across(q, s, e).wait_recv()
        return self.PS[q, e, s, : self.cap].astype(F32) + self.R[q, e, s].astype(F32)

    def settle(self, q, s, n, *es):
        for e in es:
            for i in range(n):
                self.S[q, e, s + i] = self.chip_sum(q, s + i, e).astype(BF16)
                if s == 3:
                    self.transit(q, e).start()
                elif (s + i == 1) == (e < self.half):
                    self.final(q, s + i == 2, e).start()

    def pass_on(self, q):
        for k in range(self.half):
            for e, s in ((k, 2), (k + self.half, 1)):
                self.transit(q, e).wait_recv()
                self.S[q, e, s] = (self.S[q, e, s].astype(F32) + self.T[q, e].astype(F32)).astype(BF16)
                self.final(q, s == 2, e).start()

    def gates(self):
        chunk = self.chunk
        for e in range(self.experts):
            logits = 0.0
            for q in range(2):
                weight = self.router[e : e + 1, q * chunk : (q + 1) * chunk].astype(F32)
                logits = logits + jnp.sum(self.rows[q, e].astype(F32) * weight, axis=1, keepdims=True)
            self.GT[e] = jax.nn.sigmoid(logits)

    def finish(self, q, weighted):
        for e in range(self.experts):
            total = self.chip_sum(q, 0, e)
            for up in (True, False):
                self.final(q, up, e).wait_recv()
            total = total + self.F[q, 0, e].astype(F32) + self.F[q, 1, e].astype(F32)
            weighted[q, e] = (self.GT[e] * total).astype(BF16)

    def run(self):
        half = self.half
        early, late = range(0, self.experts, half), range(1, self.experts, half)
        self.local()
        self.receive(0, *range(2 * half, 3 * half))
        self.receive(1, *range(2 * half))
        self.compute(1, 2, *early)
        self.compute(1, 2, *late)
        self.settle(0, 1, 2, *early)
        self.receive(1, *range(2 * half, 3 * half))
        self.settle(0, 1, 2, *late)
        self.compute(3, 1, *early)
        self.settle(1, 1, 2, *early)
        self.compute(3, 1, *late)
        self.settle(0, 3, 1, *early)
        self.settle(0, 3, 1, *late)
        self.settle(1, 1, 2, *late)
        self.pass_on(0)
        self.settle(1, 3, 1, *early)
        self.settle(1, 3, 1, *late)

    def drain(self):
        for q in range(2):
            for e in range(self.experts):
                self.direct(q, 1, e).wait_send()
                self.direct(q, 2, e).wait_send()
                self.onward(q, e).wait_send()
                self.final(q, True, e).wait_send()
                self.final(q, False, e).wait_send()
                self.transit(q, e).wait_send()
                for s in range(4):
                    self.across(q, s, e, s == 0).wait_send()
                    self.part_across(q, s, e).wait_send()

    @staticmethod
    def scratch(experts, cap, width, hidden):
        dma = pltpu.SemaphoreType.DMA
        chunk = width // 2
        return dict(
            X=pltpu.VMEM((2, experts, 4, 2 * cap, chunk), BF16),
            W1=pltpu.VMEM((experts, width, hidden), BF16),
            W2=pltpu.VMEM((experts, hidden, width), BF16),
            PS=pltpu.VMEM((2, experts, 4, 2 * cap, chunk), BF16),
            R=pltpu.VMEM((2, experts, 4, cap, chunk), BF16),
            S=pltpu.VMEM((2, experts, 4, cap, chunk), BF16),
            T=pltpu.VMEM((2, experts, cap, chunk), BF16),
            F=pltpu.VMEM((2, 2, experts, cap, chunk), BF16),
            GT=pltpu.VMEM((experts, cap, 1), F32),
            w_sem=dma((2, experts)),
            sendP=dma((2, 4, experts)),
            recvP=dma((2, 4, experts)),
            sendI=dma((2, 4, experts)),
            recvI=dma((2, 4, experts)),
            rsend=dma((2, 4, experts)),
            rrecv=dma((2, 4, experts)),
            fsend=dma((2, 2, experts)),
            frecv=dma((2, 2, experts)),
            tsend=dma((2, experts)),
            trecv=dma((2, experts)),
        )


class NoExperts:
    def __init__(self, rows):
        self.rows = rows

    def __getattr__(self, name):
        return lambda *_: []

    def finish(self, q, weighted):
        for e in range(self.rows.shape[1]):
            weighted[q, e] = self.rows[q, e]


def layer_kernel(
    names, with_experts, dat_count, tokens, gain, ids, picks, router, w1_hbm, w2_hbm, out, rows, weighted, *refs
):
    refs = dict(zip(names, refs))
    tok_rows, width = tokens.shape
    ex = Exchange({k: refs.pop(k) for k in Exchange.scratch(8, 8, 8)}, width)
    xp = Experts(refs, rows, router, w1_hbm, w2_hbm) if with_experts else NoExperts(rows)
    xp.load()
    barrier = pltpu.get_barrier_semaphore()
    others = ex.peers() + xp.peers()
    for other in others:
        pl.semaphore_signal(barrier, inc=1, device_id=other, device_id_type=MESH)
    ex.routes(ids, picks, tok_rows, picks.shape[0] * picks.shape[1], dat_count)
    ex.normalize(tokens, gain)
    pl.semaphore_wait(barrier, len(others))

    near, rest = pieces(0), pieces(1)
    ex.open_codes()
    ex.open_ring(*near, *rest[:2])
    ex.select(0, 0)
    ex.code_hop(1)
    ex.hop(1, *near)
    ex.open_ring(*rest[2:])
    ex.select(0, 1, 7)
    ex.code_hop(2)
    ex.hop(2, *near)
    ex.hop(1, *rest[:2])
    ex.select(0, 2, 6)
    ex.select(1, 0)
    ex.code_hop(3)
    ex.hop(3, *near)
    ex.hop(1, *rest[2:])
    ex.select(0, 3, 5)
    ex.select(1, 1, 7)
    ex.code_hop(4)
    ex.hop(4, *near)
    ex.select(0, 4)
    ex.hop(2, *rest)
    ex.select(1, 2, 6)
    ex.hop(3, *rest)
    ex.select(1, 3, 5)
    ex.compact(0, rows)
    xp.begin(0)
    ex.hop(4, *rest)
    ex.select(1, 4)
    xp.receive(0, 0, 1)
    ex.compact(1, rows)
    xp.begin(1)
    xp.receive(0, 2, 3)
    xp.gates()
    ex.expanders()
    xp.run()

    xp.finish(0, weighted)
    ex.send_back(0, weighted, FAR, 5, 3)
    xp.pass_on(1)
    ex.fold_far(0)
    ex.send_back(0, weighted, 6, 2)
    xp.finish(1, weighted)
    ex.send_back(1, weighted, FAR, 5, 3)
    ex.fold_step(0, 1)
    ex.fold_far(1)
    ex.send_back(0, weighted, 7, 1)
    ex.fold_step(0, 2)
    ex.send_back(1, weighted, 6, 2)
    ex.fold_step(1, 1)
    ex.send_back(0, weighted, 0)
    ex.fold_step(0, 3)
    ex.send_back(1, weighted, 7, 1)
    ex.drain(0)
    ex.fold_step(1, 2)
    ex.send_back(1, weighted, 0)
    xp.drain()
    ex.fold_end(0, tokens, out)
    ex.fold_step(1, 3)
    ex.fold_end(1, tokens, out)
    ex.drain(1)


def whole_layer(tokens, gain, ids, picks, router, inner_weight, outer_weight, dat_count, with_experts=True):
    tok_rows, width = tokens.shape
    experts, _, hidden = inner_weight.shape
    cap = picks.shape[1]
    vmem = pl.BlockSpec(memory_space=pltpu.VMEM)
    hbm = pl.BlockSpec(memory_space=pl.ANY)
    scratch = Exchange.scratch(tok_rows, width, experts * cap)
    if with_experts:
        scratch.update(Experts.scratch(experts, cap, width, hidden))
    slots = pltpu.VMEM((2, experts, cap, width // 2), BF16)
    return pl.pallas_call(
        functools.partial(layer_kernel, tuple(scratch), with_experts, dat_count),
        name="whole_layer",
        out_shape=jax.ShapeDtypeStruct((tok_rows, width), BF16),
        in_specs=[vmem] * 5 + [hbm] * 2,
        out_specs=vmem,
        scratch_shapes=[slots, slots] + list(scratch.values()),
        compiler_params=pltpu.CompilerParams(
            collective_id=0, has_side_effects=True, vmem_limit_bytes=60 * 1024 * 1024
        ),
    )(tokens, gain, ids, picks, router, inner_weight, outer_weight)


def body(tokens, norm_gain, router_weight, inner_weight, outer_weight, slot_tokens, slot_ids):
    return whole_layer(
        tokens, norm_gain[None, :], slot_ids.T, slot_tokens, router_weight.T, inner_weight, outer_weight,
        lax.axis_size("dat"),
    )


def solution(mesh):
    in_specs = (
        P(("exp", "dat"), None),
        P(),
        P(None, "exp"),
        P("exp", None, "dat"),
        P("exp", "dat", None),
        P("exp", "dat"),
        P(("exp", "dat"), None),
    )
    out_specs = P(("exp", "dat"), None)
    return jax.shard_map(body, mesh=mesh, in_specs=in_specs, out_specs=out_specs, check_vma=False)
```

```python
import functools

import jax
import jax.numpy as jnp
from jax import lax
from jax.experimental import pallas as pl
from jax.experimental.pallas import tpu as pltpu
from jax.sharding import PartitionSpec as P

EPSILON = 1e-06
MESH = pl.DeviceIdType.MESH
BF16 = jnp.bfloat16
F32 = jnp.float32
I32 = jnp.int32

NX, NZ, NY = 4, 8, 4
BUCKET = 24
FAR = NZ // 2
NP = 8


def dot(a, b):
    return jnp.dot(a, b, preferred_element_type=F32)


def onehot(mask):
    return mask.astype(F32).astype(BF16)


def down_rows(row):
    n = row.shape[1]
    return jnp.transpose(jnp.broadcast_to(row, (n, n)))


def count(mask):
    return jnp.sum(mask.astype(F32), axis=0, keepdims=True).astype(I32)


def remote(src, dst, send, recv, where):
    return pltpu.make_async_remote_copy(
        src_ref=src, dst_ref=dst, send_sem=send, recv_sem=recv, device_id=where, device_id_type=MESH
    )


def pieces(q):
    return list(range(q * NP // 2, (q + 1) * NP // 2))


class Exchange:
    def __init__(self, refs, width):
        self.__dict__.update(refs)
        exp = lax.axis_index("exp")
        self.x, self.z = exp // NZ, exp % NZ
        self.chunk, self.piece = width // 2, width // NP

    def at(self, dx, dz):
        return {"exp": ((self.x + dx) % NX) * NZ + (self.z + dz) % NZ}

    def peers(self):
        return [self.at(0, 1), self.at(0, NZ - 1)] + [self.at(dx, 0) for dx in range(1, NX)]

    def routes(self, slot_ids, slot_tokens, tok_rows, slots, dat_count):
        ids = [slot_ids[k : k + 1] for k in range(2)]
        owners = [row // (slots * dat_count) for row in ids]
        for k in range(2):
            rank = 0
            for m in range(2):
                rank = rank + count((down_rows(owners[m]) == owners[k]) & (down_rows(ids[m]) < ids[k]))
            self.C[0, k : k + 1] = owners[k] * BUCKET + rank
        experts = slot_tokens.shape[0]
        per = experts // 2
        source = [
            jnp.concatenate([slot_tokens[b * per + i : b * per + i + 1] for i in range(per)], axis=1)
            // (tok_rows * dat_count)
            for b in range(2)
        ]
        n = slots // 2
        earlier = lax.broadcasted_iota(I32, (n, n), 0) < lax.broadcasted_iota(I32, (n, n), 1)
        for b in range(2):
            rank = count((down_rows(source[b]) == source[b]) & earlier)
            if b == 1:
                rank = rank + count(down_rows(source[0]) == source[1])
            place = ((source[b] // NZ - self.x + NX) % NX) * NZ + (self.z - source[b] % NZ + NZ) % NZ
            self.PO[b : b + 1] = place * BUCKET + rank

    def spread(self, j, p, up):
        src = self.G.at[(j - 1) if up else (j + 1) % NZ, p]
        where = self.at(0, 1) if up else self.at(0, NZ - 1)
        return remote(src, self.G.at[j, p], self.gsend.at[j, p], self.grecv.at[j, p], where)

    def code(self, j):
        up = j <= FAR
        src = self.C.at[(j - 1) if up else (j + 1) % NZ]
        where = self.at(0, 1) if up else self.at(0, NZ - 1)
        return remote(src, self.C.at[j], self.csend.at[j], self.crecv.at[j], where)

    def open_codes(self):
        self.code(1).start()
        self.code(NZ - 1).start()

    def code_hop(self, s):
        self.code(s).wait_recv()
        if s < FAR:
            self.code(s + 1).start()
            self.code(NZ - s).wait_recv()
            if s < FAR - 1:
                self.code(NZ - s - 1).start()

    def bucket(self, ph, q, j, dx):
        there = NX - dx
        dst = self.A.at[q, there, j] if ph == 0 else self.B.at[q, j, there]
        i = dx - 1
        return remote(
            self.Q.at[ph, q, j, i], dst, self.xsend.at[ph, q, j, i], self.xrecv.at[ph, q, j, i], self.at(dx, 0)
        )

    def send_buckets(self, ph, q, j, rows):
        n = BUCKET
        for dx in (2, 1, 3):
            self.Q[ph, q, j, dx - 1] = rows[dx * n : (dx + 1) * n]
            self.bucket(ph, q, j, dx).start()
        if ph == 0:
            self.A[q, 0, j] = rows[:n]
        else:
            self.B[q, j, 0] = rows[:n]

    def landed(self, ph, q, j):
        for dx in range(1, NX):
            self.bucket(ph, q, j, dx).wait_recv()

    def row_codes(self, shape, dim):
        line = lax.broadcasted_iota(I32, shape, dim)
        dx = sum((line >= BUCKET * k).astype(I32) for k in (1, 2, 3))
        owner = ((self.x + dx) % NX) * NZ + self.z
        return jnp.where(line < BUCKET * NX, owner * BUCKET + line - BUCKET * dx, -7)

    def select(self, q, *js):
        for j in js:
            rows = self.row_codes((NX * BUCKET, self.C.shape[2]), 0)
            hit = onehot((rows == self.C[j, 0:1]) | (rows == self.C[j, 1:2]))
            parts = [dot(hit, self.G[j, p]) for p in pieces(q)]
            self.send_buckets(0, q, j, jnp.concatenate(parts, axis=1).astype(BF16))

    def normalize(self, tokens, gain):
        values = tokens[...].astype(F32)
        scale = lax.rsqrt(jnp.mean(values * values, axis=-1, keepdims=True) + EPSILON)
        normed = (values * scale * gain[...]).astype(BF16)
        for p in range(NP):
            self.G[0, p] = normed[:, p * self.piece : (p + 1) * self.piece]

    def open_ring(self, *ps):
        for p in ps:
            self.spread(1, p, True).start()
            self.spread(NZ - 1, p, False).start()

    def hop(self, s, *ps):
        for p in ps:
            for up in (True, False):
                j, onward = (s, s + 1) if up else (NZ - s, NZ - s - 1)
                far_way = up == (p % 2 == 0)
                if s < FAR or far_way:
                    self.spread(j, p, up).wait_recv()
                if s < FAR - 1 or (s == FAR - 1 and far_way):
                    self.spread(onward, p, up).start()

    def compact(self, q, rows):
        for j in range(NZ):
            self.landed(0, q, j)
        _, experts, cap, width = rows.shape
        total = NX * NZ * BUCKET
        arrived = self.A[q].reshape(total, width)
        per = experts // 2
        for b in range(2):
            places = down_rows(self.PO[b : b + 1])[:, :1]
            hit = onehot(places == lax.broadcasted_iota(I32, (per * cap, total), 1))
            got = dot(hit, arrived).astype(BF16)
            for i in range(per):
                rows[q, b * per + i] = got[i * cap : (i + 1) * cap]

    def expanders(self):
        n = self.C.shape[2]
        codes = self.row_codes((n, 128), 1)
        for j in range(NZ):
            first, second = down_rows(self.C[j, 0:1]), down_rows(self.C[j, 1:2])
            self.OT[j] = onehot((first == codes) | (second == codes))

    def send_back(self, q, weighted, *js):
        _, experts, cap, width = weighted.shape
        per = experts // 2
        line = lax.broadcasted_iota(I32, (NX * BUCKET, per * cap), 0)
        dx = sum((line >= BUCKET * k).astype(I32) for k in (1, 2, 3))
        base = dx * (NZ * BUCKET) + line - BUCKET * dx
        for j in js:
            out = 0
            for b in range(2):
                hit = onehot(base + j * BUCKET == self.PO[b : b + 1])
                out = out + dot(hit, weighted[q, b * per : (b + 1) * per].reshape(per * cap, width))
            self.send_buckets(1, q, j, out.astype(BF16))

    def part(self, j, p):
        q, h = p // (NP // 2), p % (NP // 2)
        n = NX * BUCKET
        rows = self.B[q, j, :, :, h * self.piece : (h + 1) * self.piece].reshape(n, self.piece)
        return dot(self.OT[j][:, :n], rows)

    def fold(self, j, p, up):
        where, way = (self.at(0, 1), 0) if up else (self.at(0, NZ - 1), 1)
        there = (j + 1) % NZ if up else j - 1
        return remote(
            self.V.at[j, p], self.RP.at[way, there, p], self.vsend.at[j, p], self.vrecv.at[way, there, p], where
        )

    def carried(self, j, p, up):
        self.fold((j - 1) % NZ if up else j + 1, p, up).wait_recv()
        return self.RP[0 if up else 1, j, p].astype(F32)

    def emit(self, j, p, up, incoming):
        value = self.part(j, p)
        if incoming:
            value = value + self.carried(j, p, up)
        self.V[j, p] = value.astype(BF16)
        self.fold(j, p, up).start()

    def fold_far(self, q):
        self.landed(1, q, FAR)
        for p in pieces(q):
            self.emit(FAR, p, p % 2 == 0, False)

    def fold_step(self, q, s):
        up, down = FAR + s, FAR - s
        for j in (up, down):
            self.landed(1, q, j)
        for first in (True, False):
            for p in pieces(q):
                rising = (p % 2 == 1) == first
                self.emit(up if rising else down, p, rising, s > 1 or not first)

    def fold_end(self, q, tokens, out):
        self.landed(1, q, 0)
        for p in pieces(q):
            cut = slice(p * self.piece, (p + 1) * self.piece)
            total = tokens[:, cut].astype(F32) + self.part(0, p)
            total = total + self.carried(0, p, True) + self.carried(0, p, False)
            out[:, cut] = total.astype(BF16)

    def drain(self, ph):
        for q in range(2):
            for j in range(NZ):
                for dx in range(1, NX):
                    self.bucket(ph, q, j, dx).wait_send()
        for j in range(1, NZ):
            if ph == 0:
                self.code(j).wait_send()
            for p in range(NP):
                far_up = j == FAR and p % 2 == 0
                if ph == 0:
                    self.spread(j, p, j < FAR or far_up).wait_send()
                else:
                    self.fold(j, p, j > FAR or far_up).wait_send()

    @staticmethod
    def scratch(tok_rows, width, slots):
        dma = pltpu.SemaphoreType.DMA
        chunk, piece = width // 2, width // NP
        return dict(
            G=pltpu.VMEM((NZ, NP, tok_rows, piece), BF16),
            C=pltpu.VMEM((NZ, 2, tok_rows), I32),
            PO=pltpu.VMEM((2, slots // 2), I32),
            Q=pltpu.VMEM((2, 2, NZ, NX - 1, BUCKET, chunk), BF16),
            A=pltpu.VMEM((2, NX, NZ, BUCKET, chunk), BF16),
            B=pltpu.VMEM((2, NZ, NX, BUCKET, chunk), BF16),
            OT=pltpu.VMEM((NZ, tok_rows, 128), BF16),
            V=pltpu.VMEM((NZ, NP, tok_rows, piece), BF16),
            RP=pltpu.VMEM((2, NZ, NP, tok_rows, piece), BF16),
            gsend=dma((NZ, NP)),
            grecv=dma((NZ, NP)),
            csend=dma((NZ,)),
            crecv=dma((NZ,)),
            xsend=dma((2, 2, NZ, NX - 1)),
            xrecv=dma((2, 2, NZ, NX - 1)),
            vsend=dma((NZ, NP)),
            vrecv=dma((2, NZ, NP)),
        )


class Experts:
    def __init__(self, refs, rows, router, w1_hbm, w2_hbm):
        self.__dict__.update(refs)
        self.rows, self.router, self.w1_hbm, self.w2_hbm = rows, router, w1_hbm, w2_hbm
        _, self.experts, self.cap, self.chunk = rows.shape
        self.half = self.experts // 2
        dat = lax.axis_index("dat")
        c, y = dat % 2, dat // 2
        self.partner = {"dat": y * 2 + 1 - c}
        self.plus = {"dat": ((y + 1) % NY) * 2 + c}
        self.minus = {"dat": ((y + NY - 1) % NY) * 2 + c}
        self.own, self.other = pl.ds(0, self.cap), pl.ds(self.cap, self.cap)

    def peers(self):
        return [self.partner, self.plus, self.minus]

    def weights(self, e):
        return [
            pltpu.make_async_copy(self.w1_hbm.at[e], self.W1.at[e], self.w_sem.at[0, e]),
            pltpu.make_async_copy(self.w2_hbm.at[e], self.W2.at[e], self.w_sem.at[1, e]),
        ]

    def load(self):
        for e in range(self.experts):
            for copy in self.weights(e):
                copy.start()

    def direct(self, q, s, e):
        return remote(
            self.rows.at[q, e], self.X.at[q, e, s, self.own], self.sendI.at[q, s, e], self.recvI.at[q, s, e],
            self.plus if s == 1 else self.minus,
        )

    def onward(self, q, e):
        s, where = (1, self.plus) if e < self.half else (2, self.minus)
        return remote(
            self.X.at[q, e, s, self.own], self.X.at[q, e, 3, self.own],
            self.sendI.at[q, 3, e], self.recvI.at[q, 3, e], where,
        )

    def across(self, q, s, e, own=False):
        src = self.rows.at[q, e] if own else self.X.at[q, e, s, self.own]
        return remote(
            src, self.X.at[q, e, s, self.other], self.sendP.at[q, s, e], self.recvP.at[q, s, e], self.partner
        )

    def part_across(self, q, s, e):
        return remote(
            self.PS.at[q, e, s, self.other], self.R.at[q, e, s],
            self.rsend.at[q, s, e], self.rrecv.at[q, s, e], self.partner,
        )

    def final(self, q, up, e):
        src, i, where = (self.S.at[q, e, 2], 0, self.plus) if up else (self.S.at[q, e, 1], 1, self.minus)
        return remote(src, self.F.at[q, i, e], self.fsend.at[q, i, e], self.frecv.at[q, i, e], where)

    def transit(self, q, e):
        where = self.plus if e < self.half else self.minus
        return remote(self.S.at[q, e, 3], self.T.at[q, e], self.tsend.at[q, e], self.trecv.at[q, e], where)

    def pairs(self, k):
        experts, half = self.experts, self.half
        if k < experts:
            return [(1, k), (2, (k + half) % experts)]
        if k < experts + half:
            return [(3, k - experts), (3, k - experts + half)]
        return []

    def begin(self, q):
        for e in range(self.experts):
            self.across(q, 0, e, True).start()
        for k in range(self.experts):
            for s, e in self.pairs(k):
                self.direct(q, s, e).start()
        for e in range(self.experts):
            self.X[q, e, 0, : self.cap] = self.rows[q, e]

    def receive(self, q, *ks):
        for k in ks:
            for s, e in self.pairs(k):
                copy = self.onward(q, e) if s == 3 else self.direct(q, s, e)
                copy.wait_recv()
                self.across(q, s, e).start()
                if k < self.half:
                    self.onward(q, e).start()

    def matmuls(self, e, s, n):
        chunk, tall = self.chunk, n * 2 * self.cap
        inner = 0.0
        for q in range(2):
            block = self.X[q, e, s : s + n].reshape(tall, chunk)
            inner = inner + dot(block, self.W1[e, q * chunk : (q + 1) * chunk])
        hidden = jnp.maximum(inner, 0.0).astype(BF16)
        for q in range(2):
            sums = dot(hidden, self.W2[e, :, q * chunk : (q + 1) * chunk]).astype(BF16)
            self.PS[q, e, s : s + n] = sums.reshape(n, 2 * self.cap, chunk)

    def local(self):
        def one(e, carry):
            for copy in self.weights(e):
                copy.wait()
            for q in range(2):
                self.across(q, 0, e, True).wait_recv()
            self.matmuls(e, 0, 1)
            for q in range(2):
                self.part_across(q, 0, e).start()
            return carry

        lax.fori_loop(0, self.experts, one, 0)

    def compute(self, s, n, *es):
        for e in es:
            for i in range(n):
                for q in range(2):
                    self.across(q, s + i, e).wait_recv()
        first, gap = es[0], es[1] - es[0]

        def one(i, carry):
            self.matmuls(first + gap * i, s, n)
            return carry

        lax.fori_loop(0, 2, one, 0)
        for q in range(2):
            for e in es:
                for i in range(n):
                    self.part_across(q, s + i, e).start()

    def chip_sum(self, q, s, e):
        self.part_across(q, s, e).wait_recv()
        return self.PS[q, e, s, : self.cap].astype(F32) + self.R[q, e, s].astype(F32)

    def settle(self, q, s, n, *es):
        for e in es:
            for i in range(n):
                self.S[q, e, s + i] = self.chip_sum(q, s + i, e).astype(BF16)
                if s == 3:
                    self.transit(q, e).start()
                elif (s + i == 1) == (e < self.half):
                    self.final(q, s + i == 2, e).start()

    def pass_on(self, q):
        for k in range(self.half):
            for e, s in ((k, 2), (k + self.half, 1)):
                self.transit(q, e).wait_recv()
                self.S[q, e, s] = (self.S[q, e, s].astype(F32) + self.T[q, e].astype(F32)).astype(BF16)
                self.final(q, s == 2, e).start()

    def gates(self):
        chunk = self.chunk
        for e in range(self.experts):
            logits = 0.0
            for q in range(2):
                weight = self.router[e : e + 1, q * chunk : (q + 1) * chunk].astype(F32)
                logits = logits + jnp.sum(self.rows[q, e].astype(F32) * weight, axis=1, keepdims=True)
            self.GT[e] = jax.nn.sigmoid(logits)

    def finish(self, q, weighted):
        for e in range(self.experts):
            total = self.chip_sum(q, 0, e)
            for up in (True, False):
                self.final(q, up, e).wait_recv()
            total = total + self.F[q, 0, e].astype(F32) + self.F[q, 1, e].astype(F32)
            weighted[q, e] = (self.GT[e] * total).astype(BF16)

    def run(self):
        half = self.half
        early, late = range(0, self.experts, half), range(1, self.experts, half)
        self.local()
        self.receive(0, *range(2 * half, 3 * half))
        self.receive(1, *range(2 * half))
        self.compute(1, 2, *early)
        self.compute(1, 2, *late)
        self.settle(0, 1, 2, *early)
        self.receive(1, *range(2 * half, 3 * half))
        self.settle(0, 1, 2, *late)
        self.compute(3, 1, *early)
        self.settle(1, 1, 2, *early)
        self.settle(0, 3, 1, *early)
        self.compute(3, 1, *late)
        self.settle(0, 3, 1, *late)
        self.settle(1, 1, 2, *late)
        self.pass_on(0)
        self.settle(1, 3, 1, *early)
        self.settle(1, 3, 1, *late)

    def drain(self):
        for q in range(2):
            for e in range(self.experts):
                self.direct(q, 1, e).wait_send()
                self.direct(q, 2, e).wait_send()
                self.onward(q, e).wait_send()
                self.final(q, True, e).wait_send()
                self.final(q, False, e).wait_send()
                self.transit(q, e).wait_send()
                for s in range(4):
                    self.across(q, s, e, s == 0).wait_send()
                    self.part_across(q, s, e).wait_send()

    @staticmethod
    def scratch(experts, cap, width, hidden):
        dma = pltpu.SemaphoreType.DMA
        chunk = width // 2
        return dict(
            X=pltpu.VMEM((2, experts, 4, 2 * cap, chunk), BF16),
            W1=pltpu.VMEM((experts, width, hidden), BF16),
            W2=pltpu.VMEM((experts, hidden, width), BF16),
            PS=pltpu.VMEM((2, experts, 4, 2 * cap, chunk), BF16),
            R=pltpu.VMEM((2, experts, 4, cap, chunk), BF16),
            S=pltpu.VMEM((2, experts, 4, cap, chunk), BF16),
            T=pltpu.VMEM((2, experts, cap, chunk), BF16),
            F=pltpu.VMEM((2, 2, experts, cap, chunk), BF16),
            GT=pltpu.VMEM((experts, cap, 1), F32),
            w_sem=dma((2, experts)),
            sendP=dma((2, 4, experts)),
            recvP=dma((2, 4, experts)),
            sendI=dma((2, 4, experts)),
            recvI=dma((2, 4, experts)),
            rsend=dma((2, 4, experts)),
            rrecv=dma((2, 4, experts)),
            fsend=dma((2, 2, experts)),
            frecv=dma((2, 2, experts)),
            tsend=dma((2, experts)),
            trecv=dma((2, experts)),
        )


class NoExperts:
    def __init__(self, rows):
        self.rows = rows

    def __getattr__(self, name):
        return lambda *_: []

    def finish(self, q, weighted):
        for e in range(self.rows.shape[1]):
            weighted[q, e] = self.rows[q, e]


def layer_kernel(
    names, with_experts, dat_count, tokens, gain, ids, picks, router, w1_hbm, w2_hbm, out, rows, weighted, *refs
):
    refs = dict(zip(names, refs))
    tok_rows, width = tokens.shape
    ex = Exchange({k: refs.pop(k) for k in Exchange.scratch(8, 8, 8)}, width)
    xp = Experts(refs, rows, router, w1_hbm, w2_hbm) if with_experts else NoExperts(rows)
    xp.load()
    barrier = pltpu.get_barrier_semaphore()
    others = ex.peers() + xp.peers()
    for other in others:
        pl.semaphore_signal(barrier, inc=1, device_id=other, device_id_type=MESH)
    ex.routes(ids, picks, tok_rows, picks.shape[0] * picks.shape[1], dat_count)
    ex.normalize(tokens, gain)
    pl.semaphore_wait(barrier, len(others))

    near, rest = pieces(0), pieces(1)
    ex.open_codes()
    ex.open_ring(*near, *rest[:2])
    ex.select(0, 0)
    ex.code_hop(1)
    ex.hop(1, *near)
    ex.open_ring(*rest[2:])
    ex.select(0, 1, 7)
    ex.code_hop(2)
    ex.hop(2, *near)
    ex.hop(1, *rest[:2])
    ex.select(0, 2, 6)
    ex.select(1, 0)
    ex.code_hop(3)
    ex.hop(3, *near)
    ex.hop(1, *rest[2:])
    ex.select(0, 3, 5)
    ex.select(1, 1, 7)
    ex.code_hop(4)
    ex.hop(4, *near)
    ex.select(0, 4)
    ex.hop(2, *rest)
    ex.select(1, 2, 6)
    ex.hop(3, *rest)
    ex.select(1, 3, 5)
    ex.compact(0, rows)
    xp.begin(0)
    ex.expanders()
    ex.hop(4, *rest)
    ex.select(1, 4)
    xp.receive(0, 0, 1)
    ex.compact(1, rows)
    xp.begin(1)
    xp.receive(0, 2, 3)
    xp.gates()
    xp.run()

    xp.finish(0, weighted)
    ex.send_back(0, weighted, FAR, 5, 3)
    xp.pass_on(1)
    ex.fold_far(0)
    ex.send_back(0, weighted, 6, 2)
    xp.finish(1, weighted)
    ex.send_back(1, weighted, FAR, 5, 3)
    ex.fold_step(0, 1)
    ex.send_back(0, weighted, 7, 1)
    ex.fold_far(1)
    ex.send_back(1, weighted, 6, 2)
    ex.fold_step(0, 2)
    ex.send_back(0, weighted, 0)
    ex.fold_step(1, 1)
    ex.send_back(1, weighted, 7, 1)
    ex.fold_step(0, 3)
    ex.send_back(1, weighted, 0)
    ex.drain(0)
    ex.fold_step(1, 2)
    xp.drain()
    ex.fold_end(0, tokens, out)
    ex.fold_step(1, 3)
    ex.drain(1)
    ex.fold_end(1, tokens, out)


def whole_layer(tokens, gain, ids, picks, router, inner_weight, outer_weight, dat_count, with_experts=True):
    tok_rows, width = tokens.shape
    experts, _, hidden = inner_weight.shape
    cap = picks.shape[1]
    vmem = pl.BlockSpec(memory_space=pltpu.VMEM)
    hbm = pl.BlockSpec(memory_space=pl.ANY)
    scratch = Exchange.scratch(tok_rows, width, experts * cap)
    if with_experts:
        scratch.update(Experts.scratch(experts, cap, width, hidden))
    slots = pltpu.VMEM((2, experts, cap, width // 2), BF16)
    return pl.pallas_call(
        functools.partial(layer_kernel, tuple(scratch), with_experts, dat_count),
        name="whole_layer",
        out_shape=jax.ShapeDtypeStruct((tok_rows, width), BF16),
        in_specs=[vmem] * 5 + [hbm] * 2,
        out_specs=vmem,
        scratch_shapes=[slots, slots] + list(scratch.values()),
        compiler_params=pltpu.CompilerParams(
            collective_id=0, has_side_effects=True, vmem_limit_bytes=60 * 1024 * 1024
        ),
    )(tokens, gain, ids, picks, router, inner_weight, outer_weight)


def body(tokens, norm_gain, router_weight, inner_weight, outer_weight, slot_tokens, slot_ids):
    return whole_layer(
        tokens, norm_gain[None, :], slot_ids.T, slot_tokens, router_weight.T, inner_weight, outer_weight,
        lax.axis_size("dat"),
    )


def solution(mesh):
    in_specs = (
        P(("exp", "dat"), None),
        P(),
        P(None, "exp"),
        P("exp", None, "dat"),
        P("exp", "dat", None),
        P("exp", "dat"),
        P(("exp", "dat"), None),
    )
    out_specs = P(("exp", "dat"), None)
    return jax.shard_map(body, mesh=mesh, in_specs=in_specs, out_specs=out_specs, check_vma=False)
```
